256 devices in a mesh: batch: 32 (over z, y), dim: 8 (over x, core).
Axes of the slice: x: 4, y: 4, z: 8, core: 2. Of those that a mesh axis runs over, the one named last changes fastest.
Arguments:
- x_start: float32 [1024], P('dim'), may hold values from 0.5 to 2
- y_start: float32 [], replicated, may hold values from -1 to 1
- z_start: float32 [1024], P('dim'), may hold values from -3 to 3
- increments: float32 [5, 8192, 1024], P(None, 'batch', 'dim'), may hold values from -2.7 to 2.7
- default_step: int32 [8192], P('batch'), may hold values from 0 to 6
- term_weight: float32 [1024], P('dim'), may hold values from -6 to 6
- w_first: bfloat16 [4, 1024, 1024], P(None, None, 'dim'), may hold values from -0.1875 to 0.1875
- w_second: bfloat16 [4, 1024, 1024], P(None, 'dim'), may hold values from -0.1875 to 0.1875
- w_third: bfloat16 [4, 1024, 1024], P(None, None, 'dim'), may hold values from -0.1875 to 0.1875
Outputs:
- loss: float32 [], replicated
- grad_y: float32 [], replicated
- grad_z: float32 [1024], P('dim')
- grad_first: bfloat16 [4, 1024, 1024], P(None, None, 'dim')
- grad_second: bfloat16 [4, 1024, 1024], P(None, 'dim')
- grad_third: bfloat16 [4, 1024, 1024], P(None, None, 'dim')
The draws below stay inside these ranges and needn't reach their ends.
Inputs may be any that keep to these rules, and one draw needn't show every extreme that they name: `default_step`: the time step at which a path defaults; 5 or more means no default within the window.
All inputs are finite; a program needn't handle non-finite values.
Results may differ from the reference program's by a relative error of at most 0.0085.
Values may be sent and summed in bfloat16 or wider, within the bound.
No kernel may reach another device: no remote copies, remote signals or barrier semaphores. Data moves between devices by JAX's collectives and lax.ppermute only.
A program may use at most 64 MiB of HBM per device.

```python
import math
import jax
import jax.numpy as jnp
from jax import lax

D = 1024
H = 1024
NETS = 4
STEPS = 5
PATHS = 8192


def with_ends(entries, rng, least, top_value):
    longest = entries.shape.index(max(entries.shape))
    spots = []
    for shift in (0, 1):
        where = [jax.random.randint(jax.random.fold_in(rng, axis), (), 0, length) for axis, length in enumerate(entries.shape)]
        where[longest] = (where[longest] + shift) % entries.shape[longest]
        spots.append(tuple(where))
    return entries.at[spots[0]].set(least).at[spots[1]].set(top_value)


def shard_levels(key, extent, split, smallest, largest):
    gain = 1.0
    for dim, blocks in split:
        heights = jax.random.uniform(jax.random.fold_in(jax.random.fold_in(key, 6), dim), (blocks,), jnp.float32, smallest / len(split), largest / len(split))
        gain = gain * jnp.repeat(jnp.exp(heights), extent[dim] // blocks).reshape((-1,) + (1,) * (len(extent) - 1 - dim))
    return gain


def centred(rng, extent, scale, reach, cuts=(), kind=jnp.bfloat16):
    entries = jax.random.normal(rng, extent, jnp.float32) * scale
    if len(cuts) > 0:
        entries = shard_levels(rng, extent, cuts, -0.22, 0.18) * entries
    return jnp.clip(entries, min=-reach, max=reach).astype(kind)


def setup_inputs(seed: int = 0) -> dict:
    streams_of = jax.random.split(jax.random.key(seed), 10)
    x_start = jnp.clip(jnp.exp(math.log(2.0) - 1.3862944 * jax.random.uniform(streams_of[0], (D,), jnp.float32) ** shard_levels(streams_of[0], (D,), ((0, 8),), -0.2, 0.2)), 0.5, 2.0)
    y_start = jnp.clip(jax.random.uniform(streams_of[1], (), jnp.float32, -1.0, 1.0), -1.0, 1.0)
    z_start = centred(streams_of[2], (D,), 0.5, 3.0, ((0, 8),), jnp.float32)
    increments = centred(streams_of[3], (STEPS, PATHS, D), 0.4472, 2.7, ((1, 32), (2, 8)), jnp.float32)
    default_step = with_ends(jax.random.randint(streams_of[4], (PATHS,), 0, STEPS + 2), jax.random.fold_in(streams_of[4], 1), 0, (STEPS + 2) - 1).astype(jnp.int32)
    term_weight = centred(streams_of[5], (D,), 1.0, 6.0, ((0, 8),), jnp.float32)
    w_first = centred(streams_of[6], (NETS, D, H), D ** -0.5, 0.1875, ((2, 8),))
    w_second = centred(streams_of[7], (NETS, H, H), H ** -0.5, 0.1875, ((1, 8),))
    w_third = centred(streams_of[8], (NETS, H, D), H ** -0.5, 0.1875, ((2, 8),))
    return {"x_start": x_start, "y_start": y_start, "z_start": z_start, "increments": increments, "default_step": default_step, "term_weight": term_weight, "w_first": w_first, "w_second": w_second, "w_third": w_third}


DRIFT_RATE = 0.06
VOLATILITY = 0.2
DISCOUNT = 0.02
DEFAULT_LOSS = 1.0 / 3.0

def reference(x_start, y_start, z_start, increments, default_step, term_weight, w_first, w_second, w_third):
    steps = increments.shape[0]
    tstep = 1.0 / steps
    paths = increments.shape[1]
    scale = 1.0 / math.sqrt(paths)
    counter = jnp.arange(steps, dtype=jnp.int32)
    factors = 1.0 + DISCOUNT * tstep - DEFAULT_LOSS * (counter[:, None] == default_step[None, :]).astype(jnp.float32)
    states = jnp.broadcast_to(x_start[None, :], (paths, x_start.shape[0]))
    dots = [lax.optimization_barrier(jnp.sum(increments[0] * z_start[None, :], axis=1))]
    states = states * (1.0 + DRIFT_RATE * tstep + VOLATILITY * increments[0])
    saved = []
    for index in range(1, steps):
        inputs_bf = states.astype(jnp.bfloat16)
        tanh_first = jnp.tanh(jnp.dot(inputs_bf, w_first[index - 1], preferred_element_type=jnp.float32))
        hidden_first = tanh_first.astype(jnp.bfloat16)
        tanh_second = jnp.tanh(jnp.dot(hidden_first, w_second[index - 1], preferred_element_type=jnp.float32))
        hidden_second = tanh_second.astype(jnp.bfloat16)
        control = jnp.dot(hidden_second, w_third[index - 1], preferred_element_type=jnp.float32)
        dots.append(lax.optimization_barrier(jnp.sum(control * increments[index], axis=1)))
        saved.append((inputs_bf, tanh_first, hidden_first, tanh_second, hidden_second))
        states = states * (1.0 + DRIFT_RATE * tstep + VOLATILITY * increments[index])
    target = lax.optimization_barrier(jnp.sum(states * term_weight[None, :], axis=1)) / math.sqrt(D)
    value = jnp.broadcast_to(y_start, (paths,)).astype(jnp.float32)
    for index in range(steps):
        value = factors[index] * value + dots[index]
    error = value - target
    loss = scale * jnp.sum(error * error)
    adjoint = 2.0 * scale * error
    firsts, seconds, thirds = ([], [], [])
    for index in range(steps - 1, 0, -1):
        inputs_bf, tanh_first, hidden_first, tanh_second, hidden_second = saved[index - 1]
        d_control = (adjoint[:, None] * increments[index]).astype(jnp.bfloat16)
        thirds.append(jnp.dot(hidden_second.T, d_control, preferred_element_type=jnp.float32))
        back_second = jnp.dot(d_control, w_third[index - 1].T, preferred_element_type=jnp.float32)
        d_second = (back_second * (1.0 - tanh_second * tanh_second)).astype(jnp.bfloat16)
        seconds.append(jnp.dot(hidden_first.T, d_second, preferred_element_type=jnp.float32))
        back_first = jnp.dot(d_second, w_second[index - 1].T, preferred_element_type=jnp.float32)
        d_first = (back_first * (1.0 - tanh_first * tanh_first)).astype(jnp.bfloat16)
        firsts.append(jnp.dot(inputs_bf.T, d_first, preferred_element_type=jnp.float32))
        adjoint = adjoint * factors[index]
    grad_z = lax.optimization_barrier(jnp.sum(adjoint[:, None] * increments[0], axis=0))
    adjoint = adjoint * factors[0]
    grad_y = jnp.sum(adjoint)
    grad_first = jnp.stack(firsts[::-1]).astype(jnp.bfloat16)
    grad_second = jnp.stack(seconds[::-1]).astype(jnp.bfloat16)
    grad_third = jnp.stack(thirds[::-1]).astype(jnp.bfloat16)
    return (loss, grad_y, grad_z, grad_first, grad_second, grad_third)
```

```python
import math

import jax
import jax.numpy as jnp
from jax import lax
from jax.sharding import PartitionSpec as P

D = 1024

DRIFT_RATE = 0.06
VOLATILITY = 0.2
DISCOUNT = 0.02
DEFAULT_LOSS = 1.0 / 3.0

X, CORES, Y, Z = 4, 2, 4, 8
BF = jnp.bfloat16
F32 = jnp.float32


def x_plus(value, o):
    pairs = [(CORES * i + c, CORES * ((i + o) % X) + c) for i in range(X) for c in range(CORES)]
    return lax.ppermute(value, "dim", pairs)


def x_flip(value, bit):
    pairs = [(CORES * i + c, CORES * (i ^ bit) + c) for i in range(X) for c in range(CORES)]
    return lax.ppermute(value, "dim", pairs)


def core_swap(value):
    return lax.ppermute(value, "dim", [(i, i ^ 1) for i in range(X * CORES)])


def y_plus(value, o):
    pairs = [(Y * k + i, Y * k + (i + o) % Y) for k in range(Z) for i in range(Y)]
    return lax.ppermute(value, "batch", pairs)


def z_plus(value, o):
    pairs = [(Y * k + i, Y * ((k + o) % Z) + i) for k in range(Z) for i in range(Y)]
    return lax.ppermute(value, "batch", pairs)


def batch_flip(value, bit):
    return lax.ppermute(value, "batch", [(i, i ^ bit) for i in range(Y * Z)])


def pick(array, index):
    return lax.dynamic_index_in_dim(array, index, 0, keepdims=False)


def rolled(pieces, shift):
    n = len(pieces)
    twice = jnp.stack([*pieces, *pieces])
    return lax.dynamic_slice_in_dim(twice, (n - shift) % n, n, 0)


def dot(a, b, contract):
    return lax.dot_general(a, b, (contract, ((), ())), preferred_element_type=F32)


def scattered(value, plus, me, n):
    total = pick(value, me).astype(F32)
    got = [plus(pick(value, (me + o) % n), o) for o in range(1, n)]
    for g in got:
        total = total + g.astype(F32)
    return total


def gathered(value, plus, me, n):
    return rolled([value] + [plus(value, n - o) for o in range(1, n)], me)


def local(
    x_start, y_start, z_start, increments, default_step, term_weight, w_first, w_second, w_third
):
    steps, paths, width = increments.shape
    tstep = 1.0 / steps
    scale = 1.0 / math.sqrt(paths * lax.axis_size("batch"))
    at_dim, at_batch = lax.axis_index("dim"), lax.axis_index("batch")
    x, c = at_dim // CORES, at_dim % CORES
    z, y = at_batch // Y, at_batch % Y
    first_core = c == 0
    half = D // CORES

    counter = jnp.arange(steps, dtype=jnp.int32)
    factors = (
        1.0
        + DISCOUNT * tstep
        - DEFAULT_LOSS * (counter[:, None] == default_step[None, :]).astype(F32)
    )
    states = x_start[None, :] * (1.0 + DRIFT_RATE * tstep + VOLATILITY * increments[0])
    sends = []
    for n in range(1, steps):
        sends.append(jnp.stack([states.astype(BF), increments[n].astype(BF)]))
        states = states * (1.0 + DRIFT_RATE * tstep + VOLATILITY * increments[n])
    sends = jnp.stack(sends)
    mine = [pick(sends, x)] + [x_plus(pick(sends, (x + o) % X), o) for o in range(1, X)]

    third = w_third.reshape(X, CORES, half, width)
    own_third = lax.dynamic_index_in_dim(third, c, 1, keepdims=False)
    far_third = core_swap(lax.dynamic_index_in_dim(third, 1 - c, 1, keepdims=False))

    def of_net(w):
        return [pick(w, x)] + [x_plus(pick(w, (x + o) % X), o) for o in range(1, X)]

    third_pairs = of_net(jnp.stack([own_third, far_third], axis=1))
    first_parts = of_net(w_first)
    second_parts = of_net(w_second)
    w3 = jnp.concatenate([p[i] for p in third_pairs for i in range(CORES)], axis=1)
    w1 = jnp.concatenate(first_parts, axis=1)
    w2 = jnp.concatenate(second_parts, axis=0)

    near = jnp.stack(mine)
    far = core_swap(near)
    incs = jnp.concatenate([v[o, 1] for o in range(X) for v in (near, far)], axis=1)
    order = [0, 3, 2, 1]
    near_x = rolled([near[o, 0] for o in order], x)
    far_x = rolled([far[o, 0] for o in order], x)
    low = jnp.where(first_core, near_x, far_x)
    high = jnp.where(first_core, far_x, near_x)
    inputs = jnp.concatenate([v[i] for i in range(X) for v in (low, high)], axis=1)

    tanh_first = jnp.tanh(dot(inputs, w1, ((1,), (0,))))
    hidden_first = tanh_first.astype(BF)
    part = dot(hidden_first, w2, ((1,), (0,)))
    left, right = part[:, :half], part[:, half:]
    pre = jnp.where(first_core, left, right) + core_swap(jnp.where(first_core, right, left))
    tanh_second = jnp.tanh(pre)
    back = dot(incs, w3, ((1,), (1,)))
    dots = jnp.sum(tanh_second * back, axis=1)

    coefs = [jnp.ones((paths,), F32)]
    for n in range(steps - 1, 0, -1):
        coefs.append(coefs[-1] * factors[n])
    coefs = jnp.stack(coefs[::-1])
    coef = pick(coefs, x + 1)
    target_part = jnp.sum(states * term_weight[None, :], axis=1) / math.sqrt(D)
    first_part = jnp.sum(increments[0] * z_start[None, :], axis=1)
    total = coefs[0] * first_part - target_part + coef * dots
    total = total.reshape(2, paths // 2)
    total = total + core_swap(total)
    total = total + x_flip(total, 1)
    total = total + x_flip(total, 2)
    error = total.reshape(paths) + factors[0] * coefs[0] * y_start
    adjoint = 2.0 * scale * error
    adjoint_one = adjoint * coefs[0]
    loss = scale * jnp.sum(error * error)
    grad_y = jnp.sum(adjoint_one * factors[0])
    grad_z = jnp.sum(adjoint_one[:, None] * increments[0], axis=0)
    small = jnp.concatenate(
        [grad_z, jnp.stack([loss, grad_y]), jnp.zeros((width - 2,), F32)]
    ).reshape(2, width)
    for bit in (1, 2, 4, 8, 16):
        small = small + batch_flip(small, bit)

    weight = (adjoint * coef)[:, None]
    grad_third = dot((weight * tanh_second).astype(BF), incs, ((0,), (0,))).astype(BF)
    d_second = (weight * back * (1.0 - tanh_second * tanh_second)).astype(BF)
    d_far = core_swap(d_second)
    d_all = jnp.concatenate(
        [jnp.where(first_core, d_second, d_far), jnp.where(first_core, d_far, d_second)], axis=1
    )
    grad_second = dot(hidden_first, d_all, ((0,), (0,))).astype(BF)
    d_first = (dot(d_all, w2, ((1,), (1,))) * (1.0 - tanh_first * tanh_first)).astype(BF)
    grad_first = dot(inputs, d_first, ((0,), (0,))).astype(BF)

    rows = D // (Y * Z)
    a = grad_first.reshape(Y, Z, rows, half)
    b = jnp.moveaxis(grad_second.reshape(half, Z, D // Z), 1, 0).reshape(Z, X, Y, rows, D // Z)
    e = grad_third.reshape(Y, Z, rows // 2, D)
    a = scattered(a, y_plus, y, Y).astype(BF)
    e = scattered(e, y_plus, y, Y).astype(BF)
    b = scattered(b, z_plus, z, Z).astype(BF)
    a = scattered(a, z_plus, z, Z).astype(BF)
    e = scattered(e, z_plus, z, Z).astype(BF)
    b = scattered(jnp.moveaxis(b, 1, 0), y_plus, y, Y).astype(BF)

    e = e.reshape(rows // 2, X, CORES, width).transpose(2, 1, 0, 3)
    e_far = core_swap(e[1])
    e = jnp.stack([jnp.where(first_core, e[0], e_far), jnp.where(first_core, e_far, e[0])], axis=1)
    a = a.reshape(rows, X, width).transpose(1, 0, 2)
    blocks = jnp.stack([a, e.reshape(X, rows, width), b], axis=1)
    arrived = rolled([blocks[0]] + [x_plus(blocks[o], X - o) for o in range(1, X)], x)
    two, one = arrived[:, :2], arrived[:, 2]
    two = gathered(gathered(two, z_plus, z, Z), y_plus, y, Y)
    one = gathered(gathered(one, y_plus, y, Y), z_plus, z, Z)
    out_first = two[:, :, :, 0].transpose(2, 0, 1, 3, 4).reshape(X, D, width)
    out_third = (
        two[:, :, :, 1]
        .reshape(Y, Z, X, CORES, rows // 2, width)
        .transpose(2, 3, 0, 1, 4, 5)
        .reshape(X, D, width)
    )
    out_second = one.transpose(2, 1, 3, 0, 4).reshape(X, Y * rows, D)
    return small[1, 0], small[1, 1], small[0], out_first, out_second, out_third


def solution(mesh):
    placed = (
        P("dim"),
        P(),
        P("dim"),
        P(None, "batch", "dim"),
        P("batch"),
        P("dim"),
        P(None, None, "dim"),
        P(None, "dim", None),
        P(None, None, "dim"),
    )
    return jax.shard_map(
        local,
        mesh=mesh,
        in_specs=placed,
        out_specs=(
            P(),
            P(),
            P("dim"),
            P(None, None, "dim"),
            P(None, "dim", None),
            P(None, None, "dim"),
        ),
        check_vma=False,
    )
```

```python
import math

import jax
import jax.numpy as jnp
from jax import lax
from jax.experimental import pallas as pl
from jax.experimental.pallas import tpu as pltpu
from jax.sharding import Mesh
from jax.sharding import PartitionSpec as P

D = 1024

DRIFT_RATE = 0.06
VOLATILITY = 0.2
DISCOUNT = 0.02
DEFAULT_LOSS = 1.0 / 3.0

X, CORES, Y, Z = 4, 2, 4, 8
W = D // (X * CORES)
BF = jnp.bfloat16
F32 = jnp.float32


def shifted(value, axis, n, o):
    return lax.ppermute(value, axis, [(i, (i + o) % n) for i in range(n)])


def flipped(value, axis, n, bit):
    return lax.ppermute(value, axis, [(i, i ^ bit) for i in range(n)])


def x_plus(value, o):
    return shifted(value, "x", X, o)


def y_plus(value, o):
    return shifted(value, "y", Y, o)


def core_swap(value):
    return flipped(value, "core", CORES, 1)


def exchanged(value, axis):
    return lax.all_to_all(value, axis, split_axis=0, concat_axis=0, tiled=True)


def pick(array, index):
    return lax.dynamic_index_in_dim(array, index, 0, keepdims=False)


def rolled(pieces, shift):
    n = len(pieces)
    twice = jnp.stack([*pieces, *pieces])
    return lax.dynamic_slice_in_dim(twice, (n - shift) % n, n, 0)


def dot(a, b, contract):
    return lax.dot_general(a, b, (contract, ((), ())), preferred_element_type=F32)


def vmem_call(kernel, place, args, outs, scratch=()):
    vmem = pl.BlockSpec(memory_space=pltpu.VMEM)
    return pl.pallas_call(
        kernel,
        out_shape=[jax.ShapeDtypeStruct(shape, dtype) for shape, dtype in outs],
        in_specs=[pl.BlockSpec(memory_space=pltpu.SMEM)] + [vmem] * len(args),
        out_specs=[vmem] * len(outs),
        scratch_shapes=list(scratch),
        name=kernel.__name__,
    )(place, *args)


def two_words(value):
    high = value.astype(BF).astype(F32)
    return jnp.concatenate([high, value - high], axis=0).astype(BF)


def second_kernel(place, tanh_ref, own_ref, far_ref, small_ref, out_ref, all_ref):
    half = own_ref.shape[1]

    @pl.when(place[1] == 0)
    def _():
        all_ref[:, :half] = own_ref[...]
        all_ref[:, half:] = far_ref[...]

    @pl.when(place[1] != 0)
    def _():
        all_ref[:, :half] = far_ref[...]
        all_ref[:, half:] = own_ref[...]

    hidden = tanh_ref[...].astype(BF)
    small = two_words(small_ref[...])
    for k in range(0, Z, 2):
        g = dot(hidden, all_ref[:, W * k : W * (k + 2)], ((0,), (0,)))
        for i in range(2):
            out_ref[k + i, :half, :] = g[:, W * i : W * (i + 1)].astype(BF)
            out_ref[k + i, half:, :] = small


def others_kernel(place, in_ref, tanh_ref, all_ref, w2_ref, wt_ref, inc_ref, *outs):
    tanh = tanh_ref[...]
    back = dot(all_ref[...], w2_ref[...], ((1,), (1,)))
    d_first = (back * (1.0 - tanh * tanh)).astype(BF)
    for r, out in enumerate(outs):
        to = lax.rem(place[2] + r, Y)
        g = dot(in_ref[:, pl.ds(pl.multiple_of(to * 256, 256), 256)], d_first, ((0,), (0,)))
        for k in range(Z):
            for o in range(X):
                out[k, 32 * o : 32 * o + 32, :] = g[32 * k : 32 * k + 32, W * o : W * o + W].astype(BF)
        e = dot(wt_ref[:, pl.ds(pl.multiple_of(to * 128, 128), 128)], inc_ref[...], ((0,), (0,)))
        for k in range(Z):
            for q in range(X * CORES):
                row = 128 + 16 * q
                out[k, row : row + 16, :] = e[16 * k : 16 * k + 16, W * q : W * q + W].astype(BF)


def sum_y_kernel(place, a0, a1, a2, a3, out):
    def body(k, carry):
        out[k] = (
            (a0[k].astype(F32) + a2[k].astype(F32)) + (a1[k].astype(F32) + a3[k].astype(F32))
        ).astype(BF)
        return carry

    lax.fori_loop(0, Z, body, 0)


def sum_z_kernel(place, b_ref, o0, o1, o2, o3, total):
    rows = b_ref.shape[1]

    def body(i, carry):
        at = pl.ds(pl.multiple_of(i * 16, 16), 16)
        acc = b_ref[0, at, :].astype(F32)
        for k in range(1, Z):
            acc = acc + b_ref[k, at, :].astype(F32)
        total[at, :] = acc
        return carry

    lax.fori_loop(0, rows // 16, body, 0)
    small = two_words(total[rows - 16 : rows - 8, :] + total[rows - 8 : rows, :])
    for r, out in enumerate((o0, o1, o2, o3)):
        to = lax.rem(place[2] + r, Y)
        for o in range(X):
            at = pl.ds(pl.multiple_of(128 * o + 32 * to, 32), 32)
            out[32 * o : 32 * o + 32, :] = total[at, :].astype(BF)
        out[128:, :] = small


def blocks_kernel(place, a_ref, b0, b1, b2, b3, out, small):
    x, c = place[0], place[1]
    acc = a_ref[0].astype(F32)
    for k in range(1, Z):
        acc = acc + a_ref[k].astype(F32)
    acc = acc.astype(BF)
    b = (b0[...].astype(F32) + b2[...].astype(F32)) + (b1[...].astype(F32) + b3[...].astype(F32))
    small[...] = b[128:136] + b[136:144]
    b = b[:128].astype(BF)
    for o in range(X):
        to = lax.rem(x + (X - o), X)
        own, far = CORES * to + c, CORES * to + 1 - c
        third = 128 + 32 * o
        out[own, :32, :] = acc[32 * o : 32 * o + 32]
        out[own, 32:64, :] = b[32 * o : 32 * o + 32]
        out[own, 64:, :] = acc[third : third + 16]
        out[far, :64, :] = jnp.zeros((64, W), BF)
        out[far, 64:, :] = acc[third + 16 : third + 32]


def copies_kernel(place, got, a_ref, b_ref):
    c = place[1]
    for n in range(X):
        own = CORES * n + c
        first = got[own, :32, :]
        b_ref[32 * n : 32 * n + 32, :] = got[own, 32:64, :]
        for k in range(Z):
            a_ref[k, 64 * n : 64 * n + 32, :] = first
            for h in range(CORES):
                row = 64 * n + 32 + 16 * h
                a_ref[k, row : row + 16, :] = got[CORES * n + h, 64:, :]


def out_kernel(place, a0, a1, a2, a3, b_ref, first, second, third, sems):
    copies = []

    def start(source, target):
        copy = pltpu.make_async_copy(source, target, sems.at[len(copies)])
        copy.start()
        copies.append(copy)

    for r, a in enumerate((a0, a1, a2, a3)):
        at = lax.rem(place[2] + (Y - r), Y)
        for n in range(X):
            start(a.at[:, pl.ds(64 * n, 32), :], first.at[n, at])
            for h in range(CORES):
                start(a.at[:, pl.ds(64 * n + 32 + 16 * h, 16), :], third.at[n, h, at])
        for k in range(Z):
            start(b_ref.at[k, r], second.at[:, at, :, pl.ds(W * k, W)])
    for copy in copies:
        copy.wait()


def local(
    x_start, y_start, z_start, increments, default_step, term_weight, w_first, w_second, w_third
):
    steps, paths, width = increments.shape
    tstep = 1.0 / steps
    scale = 1.0 / math.sqrt(paths * Y * Z)
    x, c, y, z = (lax.axis_index(name) for name in ("x", "core", "y", "z"))
    place = jnp.stack([x, c, y, z]).astype(jnp.int32)
    first_core = c == 0
    half = D // CORES

    counter = jnp.arange(steps, dtype=jnp.int32)
    factors = (
        1.0
        + DISCOUNT * tstep
        - DEFAULT_LOSS * (counter[:, None] == default_step[None, :]).astype(F32)
    )
    states = x_start[None, :] * (1.0 + DRIFT_RATE * tstep + VOLATILITY * increments[0])
    sends = []
    for n in range(1, steps):
        sends.append(jnp.stack([states.astype(BF), increments[n].astype(BF)]))
        states = states * (1.0 + DRIFT_RATE * tstep + VOLATILITY * increments[n])
    sends = jnp.stack(sends)
    mine = [pick(sends, x)] + [x_plus(pick(sends, (x + o) % X), o) for o in range(1, X)]

    third = w_third.reshape(X, CORES, half, width)
    own_third = lax.dynamic_index_in_dim(third, c, 1, keepdims=False)
    far_third = core_swap(lax.dynamic_index_in_dim(third, 1 - c, 1, keepdims=False))

    def of_net(w):
        return [pick(w, x)] + [x_plus(pick(w, (x + o) % X), o) for o in range(1, X)]

    third_pairs = of_net(jnp.stack([own_third, far_third], axis=1))
    first_parts = of_net(w_first)
    second_parts = of_net(w_second)
    w3 = jnp.concatenate([p[i] for p in third_pairs for i in range(CORES)], axis=1)
    w1 = jnp.concatenate(first_parts, axis=1)
    w2 = jnp.concatenate(second_parts, axis=0)

    near = jnp.stack(mine)
    far = core_swap(near)
    incs = jnp.concatenate([v[o, 1] for o in range(X) for v in (near, far)], axis=1)
    order = [0, 3, 2, 1]
    near_x = rolled([near[o, 0] for o in order], x)
    far_x = rolled([far[o, 0] for o in order], x)
    low = jnp.where(first_core, near_x, far_x)
    high = jnp.where(first_core, far_x, near_x)
    inputs = jnp.concatenate([v[i] for i in range(X) for v in (low, high)], axis=1)

    tanh_first = jnp.tanh(dot(inputs, w1, ((1,), (0,))))
    hidden_first = tanh_first.astype(BF)
    part = dot(hidden_first, w2, ((1,), (0,)))
    left, right = part[:, :half], part[:, half:]
    pre = jnp.where(first_core, left, right) + core_swap(jnp.where(first_core, right, left))
    tanh_second = jnp.tanh(pre)
    back = dot(incs, w3, ((1,), (1,)))
    dots = jnp.sum(tanh_second * back, axis=1)

    coefs = [jnp.ones((paths,), F32)]
    for n in range(steps - 1, 0, -1):
        coefs.append(coefs[-1] * factors[n])
    coefs = jnp.stack(coefs[::-1])
    coef = pick(coefs, x + 1)
    target_part = jnp.sum(states * term_weight[None, :], axis=1) / math.sqrt(D)
    first_part = jnp.sum(increments[0] * z_start[None, :], axis=1)
    total = coefs[0] * first_part - target_part + coef * dots
    total = total.reshape(2, paths // 2)
    total = total + core_swap(total)
    total = total + flipped(total, "x", X, 1)
    total = total + flipped(total, "x", X, 2)
    error = total.reshape(paths) + factors[0] * coefs[0] * y_start
    adjoint = 2.0 * scale * error
    adjoint_one = adjoint * coefs[0]
    loss = scale * jnp.sum(error * error)
    grad_y = jnp.sum(adjoint_one * factors[0])
    grad_z = jnp.sum(adjoint_one[:, None] * increments[0], axis=0)
    small = jnp.concatenate(
        [grad_z, jnp.stack([loss, grad_y]), jnp.zeros((7 * width - 2,), F32)]
    ).reshape(8, width)

    weight = (adjoint * coef)[:, None]
    weighted = (weight * tanh_second).astype(BF)
    d_second = (weight * back * (1.0 - tanh_second * tanh_second)).astype(BF)
    d_far = core_swap(d_second)
    b, d_all = vmem_call(
        second_kernel,
        place,
        (tanh_first, d_second, d_far, small),
        (((Z, half + 16, width), BF), ((paths, D), BF)),
    )
    b = exchanged(b, "z")
    a = vmem_call(
        others_kernel,
        place,
        (inputs, tanh_first, d_all, w2, weighted, incs),
        [((Z, 256, width), BF)] * Y,
    )
    a = [a[0]] + [y_plus(a[r], r) for r in range(1, Y)]
    (a,) = vmem_call(sum_y_kernel, place, a, [((Z, 256, width), BF)])
    a = exchanged(a, "z")
    b = vmem_call(
        sum_z_kernel,
        place,
        (b,),
        [((144, width), BF)] * Y,
        [pltpu.VMEM((half + 16, width), F32)],
    )
    b = [b[0]] + [y_plus(b[r], r) for r in range(1, Y)]
    blocks, small = vmem_call(
        blocks_kernel, place, (a, *b), (((X * CORES, 80, width), BF), ((8, width), F32))
    )
    arrived = exchanged(blocks, ("x", "core"))
    a, b = vmem_call(
        copies_kernel, place, (arrived,), (((Z, 256, width), BF), ((128, width), BF))
    )
    a = exchanged(a, "z")
    b = jnp.stack([b] + [y_plus(b, r) for r in range(1, Y)])
    b = exchanged(jnp.broadcast_to(b, (Z, *b.shape)), "z")
    a = [a] + [y_plus(a, r) for r in range(1, Y)]
    anywhere = pl.BlockSpec(memory_space=pl.ANY)
    first, second, third = pl.pallas_call(
        out_kernel,
        out_shape=[
            jax.ShapeDtypeStruct((X, Y, Z, 32, width), BF),
            jax.ShapeDtypeStruct((X, Y, 32, D), BF),
            jax.ShapeDtypeStruct((X, CORES, Y, Z, 16, width), BF),
        ],
        in_specs=[pl.BlockSpec(memory_space=pltpu.SMEM)] + [anywhere] * (Y + 1),
        out_specs=[anywhere] * 3,
        scratch_shapes=[pltpu.SemaphoreType.DMA((Y * (X * 3 + Z),))],
        name="out_kernel",
    )(place, *a, b.reshape(Z, Y, X, 32, width))
    return (
        small[1, 0],
        small[1, 1],
        small[0],
        first.reshape(X, D, width),
        second.reshape(X, width, D),
        third.reshape(X, D, width),
    )


def solution(mesh):
    axes = Mesh(mesh.devices.reshape(Z, Y, X, CORES), ("z", "y", "x", "core"))
    batch, dim = ("z", "y"), ("x", "core")
    placed = (
        P(dim),
        P(),
        P(dim),
        P(None, batch, dim),
        P(batch),
        P(dim),
        P(None, None, dim),
        P(None, dim, None),
        P(None, None, dim),
    )
    return jax.shard_map(
        local,
        mesh=axes,
        in_specs=placed,
        out_specs=(
            P(),
            P(),
            P(dim),
            P(None, None, dim),
            P(None, dim, None),
            P(None, None, dim),
        ),
        check_vma=False,
    )
```

```python
import math

import jax
import jax.numpy as jnp
from jax import lax
from jax.experimental import pallas as pl
from jax.experimental.pallas import tpu as pltpu
from jax.sharding import Mesh
from jax.sharding import PartitionSpec as P

D = 1024

DRIFT_RATE = 0.06
VOLATILITY = 0.2
DISCOUNT = 0.02
DEFAULT_LOSS = 1.0 / 3.0

X, CORES, Y, Z = 4, 2, 4, 8
W = D // (X * CORES)
BF = jnp.bfloat16
F32 = jnp.float32


def shifted(value, axis, n, o):
    return lax.ppermute(value, axis, [(i, (i + o) % n) for i in range(n)])


def flipped(value, axis, n, bit):
    return lax.ppermute(value, axis, [(i, i ^ bit) for i in range(n)])


def x_plus(value, o):
    return shifted(value, "x", X, o)


def y_plus(value, o):
    return shifted(value, "y", Y, o)


def core_swap(value):
    return flipped(value, "core", CORES, 1)


def exchanged(value, axis):
    return lax.all_to_all(value, axis, split_axis=0, concat_axis=0, tiled=True)


def pick(array, index):
    return lax.dynamic_index_in_dim(array, index, 0, keepdims=False)


def rolled(pieces, shift):
    n = len(pieces)
    twice = jnp.stack([*pieces, *pieces])
    return lax.dynamic_slice_in_dim(twice, (n - shift) % n, n, 0)


def dot(a, b, contract):
    return lax.dot_general(a, b, (contract, ((), ())), preferred_element_type=F32)


def vmem_call(kernel, place, args, outs, scratch=()):
    vmem = pl.BlockSpec(memory_space=pltpu.VMEM)
    return pl.pallas_call(
        kernel,
        out_shape=[jax.ShapeDtypeStruct(shape, dtype) for shape, dtype in outs],
        in_specs=[pl.BlockSpec(memory_space=pltpu.SMEM)] + [vmem] * len(args),
        out_specs=[vmem] * len(outs),
        scratch_shapes=list(scratch),
        name=kernel.__name__,
    )(place, *args)


def two_words(value):
    high = value.astype(BF).astype(F32)
    return jnp.concatenate([high, value - high], axis=0).astype(BF)


def put_sums(out, halves, to, in_ref, hid_ref, all_ref, d_first, wt_ref, inc_ref, added=None):
    g1 = dot(in_ref[:, pl.ds(pl.multiple_of(to * 256, 256), 256)], d_first, ((0,), (0,)))
    g3 = dot(wt_ref[:, pl.ds(pl.multiple_of(to * 128, 128), 128)], inc_ref[...], ((0,), (0,)))
    g2 = dot(hid_ref[...], all_ref[:, pl.ds(pl.multiple_of(to * 256, 256), 256)], ((0,), (0,)))

    def put(k, row, value):
        rows = value.shape[0]
        if added is not None and k in added[1]:
            value = value + added[0][k - added[1][0], row : row + rows, :].astype(F32)
        ref, at = (out, k) if halves is None else (out[k // halves], k % halves)
        ref[at, row : row + rows, :] = value.astype(BF)

    for k in range(Z):
        for o in range(X):
            put(k, 32 * o, g1[32 * k : 32 * k + 32, W * o : W * o + W])
            for i in range(2):
                at = W * o + 16 * k
                put(k, 256 + 32 * o + 16 * i, g2[at : at + 16, W * i : W * i + W])
        for q in range(X * CORES):
            put(k, 128 + 16 * q, g3[16 * k : 16 * k + 16, W * q : W * q + W])


def far_kernel(
    place, in_ref, tanh_ref, own_ref, far_ref, w2_ref, wt_ref, inc_ref, low, high, all_ref, d1_ref, hid_ref
):
    half = own_ref.shape[1]

    @pl.when(place[1] == 0)
    def _():
        all_ref[:, :half] = own_ref[...]
        all_ref[:, half:] = far_ref[...]

    @pl.when(place[1] != 0)
    def _():
        all_ref[:, :half] = far_ref[...]
        all_ref[:, half:] = own_ref[...]

    tanh = tanh_ref[...]
    hid_ref[...] = tanh.astype(BF)
    back = dot(all_ref[...], w2_ref[...], ((1,), (1,)))
    d_first = (back * (1.0 - tanh * tanh)).astype(BF)
    d1_ref[...] = d_first
    to = lax.rem(place[2] + 2, Y)
    put_sums((low, high), Z // 2, to, in_ref, hid_ref, all_ref, d_first, wt_ref, inc_ref)


def own_kernel(place, in_ref, hid_ref, all_ref, d1_ref, wt_ref, inc_ref, out):
    put_sums(out, None, place[2], in_ref, hid_ref, all_ref, d1_ref[...], wt_ref, inc_ref)


def near_kernel(
    place, in_ref, hid_ref, all_ref, d1_ref, wt_ref, inc_ref, from_low, from_high, up, down
):
    rest = (in_ref, hid_ref, all_ref, d1_ref[...], wt_ref, inc_ref)
    put_sums(up, None, lax.rem(place[2] + 1, Y), *rest, (from_low, range(Z // 2)))
    put_sums(down, None, lax.rem(place[2] + Y - 1, Y), *rest, (from_high, range(Z // 2, Z)))


def sum_y_kernel(place, own, from_below, from_above, small_ref, out):
    rows = own.shape[1]
    small = two_words(small_ref[...])
    for k in range(Z):
        out[k, :rows, :] = (
            own[k].astype(F32) + from_below[k].astype(F32) + from_above[k].astype(F32)
        ).astype(BF)
        out[k, rows:, :] = small


def blocks_kernel(place, a_ref, out, small):
    x, c = place[0], place[1]

    def total(row, rows):
        acc = a_ref[0, row : row + rows, :].astype(F32)
        for k in range(1, Z):
            acc = acc + a_ref[k, row : row + rows, :].astype(F32)
        return acc

    words = total(384, 16)
    small[...] = words[:8] + words[8:]
    for o in range(X):
        to = lax.rem(x + (X - o), X)
        own, far = CORES * to + c, CORES * to + 1 - c
        out[own, :32, :] = total(32 * o, 32).astype(BF)
        out[own, 32:64, :] = total(256 + 32 * o, 32).astype(BF)
        third = total(128 + 32 * o, 32).astype(BF)
        out[own, 64:, :] = third[:16]
        out[far, :64, :] = jnp.zeros((64, W), BF)
        out[far, 64:, :] = third[16:]


def pieces_kernel(place, got, out):
    c = place[1]
    for n in range(X):
        own = CORES * n + c
        out[96 * n : 96 * n + 32, :] = got[own, :32, :]
        for h in range(CORES):
            row = 96 * n + 32 + 16 * h
            out[row : row + 16, :] = got[CORES * n + h, 64:, :]
        out[96 * n + 64 : 96 * n + 96, :] = got[own, 32:64, :]


def out_kernel(place, own, below, above, low, high, first, second, third):
    y = place[2]
    parts = [(own, 0, k, k) for k in range(Z)]
    parts += [(below, Y - 1, k, k) for k in range(Z)] + [(above, 1, k, k) for k in range(Z)]
    parts += [(low, 2, k, k) for k in range(Z // 2)]
    parts += [(high, 2, k, k + Z // 2) for k in range(Z // 2)]
    for ref, off, i, k in parts:
        at = lax.rem(y + off, Y)
        for n in range(X):
            first[n, at, k] = ref[i, 96 * n : 96 * n + 32, :]
            for h in range(CORES):
                row = 96 * n + 32 + 16 * h
                third[n, h, at, k] = ref[i, row : row + 16, :]
                lane = pl.ds(pl.multiple_of(2 * W * at + W * h, W), W)
                second[n, k, :, lane] = ref[i, row + 32 : row + 48, :]


def local(
    x_start, y_start, z_start, increments, default_step, term_weight, w_first, w_second, w_third
):
    steps, paths, width = increments.shape
    tstep = 1.0 / steps
    scale = 1.0 / math.sqrt(paths * Y * Z)
    x, c, y, z = (lax.axis_index(name) for name in ("x", "core", "y", "z"))
    place = jnp.stack([x, c, y, z]).astype(jnp.int32)
    first_core = c == 0
    half = D // CORES

    counter = jnp.arange(steps, dtype=jnp.int32)
    factors = (
        1.0
        + DISCOUNT * tstep
        - DEFAULT_LOSS * (counter[:, None] == default_step[None, :]).astype(F32)
    )
    states = x_start[None, :] * (1.0 + DRIFT_RATE * tstep + VOLATILITY * increments[0])
    sends = []
    for n in range(1, steps):
        sends.append(jnp.stack([states.astype(BF), increments[n].astype(BF)]))
        states = states * (1.0 + DRIFT_RATE * tstep + VOLATILITY * increments[n])
    sends = jnp.stack(sends)
    mine = [pick(sends, x)] + [x_plus(pick(sends, (x + o) % X), o) for o in range(1, X)]

    third = w_third.reshape(X, CORES, half, width)
    own_third = lax.dynamic_index_in_dim(third, c, 1, keepdims=False)
    far_third = core_swap(lax.dynamic_index_in_dim(third, 1 - c, 1, keepdims=False))

    def of_net(w, ways):
        apart = pick(w, (x + 2) % X)
        if len(ways) == 2:
            relayed = jnp.stack([x_plus(x_plus(apart[i], o), o) for i, o in enumerate(ways)])
        else:
            relayed = x_plus(x_plus(apart, ways[0]), ways[0])
        return [
            pick(w, x),
            x_plus(pick(w, (x + 1) % X), 1),
            relayed,
            x_plus(pick(w, (x + 3) % X), 3),
        ]

    first_parts = of_net(w_first, (1,))
    second_parts = of_net(w_second, (3,))
    third_pairs = of_net(jnp.stack([own_third, far_third], axis=1), (1, 3))
    w3 = jnp.concatenate([p[i] for p in third_pairs for i in range(CORES)], axis=1)
    w1 = jnp.concatenate(first_parts, axis=1)
    w2 = jnp.concatenate(second_parts, axis=0)

    near = jnp.stack(mine)
    far = core_swap(near)
    incs = jnp.concatenate([v[o, 1] for o in range(X) for v in (near, far)], axis=1)
    order = [0, 3, 2, 1]
    near_x = rolled([near[o, 0] for o in order], x)
    far_x = rolled([far[o, 0] for o in order], x)
    low = jnp.where(first_core, near_x, far_x)
    high = jnp.where(first_core, far_x, near_x)
    inputs = jnp.concatenate([v[i] for i in range(X) for v in (low, high)], axis=1)

    tanh_first = jnp.tanh(dot(inputs, w1, ((1,), (0,))))
    hidden_first = tanh_first.astype(BF)
    part = dot(hidden_first, w2, ((1,), (0,)))
    left, right = part[:, :half], part[:, half:]
    pre = jnp.where(first_core, left, right) + core_swap(jnp.where(first_core, right, left))
    tanh_second = jnp.tanh(pre)
    back = dot(incs, w3, ((1,), (1,)))
    dots = jnp.sum(tanh_second * back, axis=1)

    coefs = [jnp.ones((paths,), F32)]
    for n in range(steps - 1, 0, -1):
        coefs.append(coefs[-1] * factors[n])
    coefs = jnp.stack(coefs[::-1])
    coef = pick(coefs, x + 1)
    target_part = jnp.sum(states * term_weight[None, :], axis=1) / math.sqrt(D)
    first_part = jnp.sum(increments[0] * z_start[None, :], axis=1)
    total = coefs[0] * first_part - target_part + coef * dots
    total = total.reshape(2, paths // 2)
    total = total + core_swap(total)
    total = total + flipped(total, "x", X, 1)
    total = total + flipped(total, "x", X, 2)
    error = total.reshape(paths) + factors[0] * coefs[0] * y_start
    adjoint = 2.0 * scale * error
    adjoint_one = adjoint * coefs[0]
    loss = scale * jnp.sum(error * error)
    grad_y = jnp.sum(adjoint_one * factors[0])
    grad_z = jnp.sum(adjoint_one[:, None] * increments[0], axis=0)
    small = jnp.concatenate(
        [grad_z, jnp.stack([loss, grad_y]), jnp.zeros((7 * width - 2,), F32)]
    ).reshape(8, width)

    weight = (adjoint * coef)[:, None]
    weighted = (weight * tanh_second).astype(BF)
    d_second = (weight * back * (1.0 - tanh_second * tanh_second)).astype(BF)
    d_far = core_swap(d_second)
    low, high, d_all, d_first, hidden = vmem_call(
        far_kernel,
        place,
        (inputs, tanh_first, d_second, d_far, w2, weighted, incs),
        (
            ((Z // 2, 384, width), BF),
            ((Z // 2, 384, width), BF),
            ((paths, D), BF),
            ((paths, half), BF),
            ((paths, half), BF),
        ),
    )
    low, high = y_plus(low, 1), y_plus(high, 3)
    shared = (inputs, hidden, d_all, d_first, weighted, incs)
    piece = ((Z, 384, width), BF)
    (own,) = vmem_call(own_kernel, place, shared, (piece,))
    up, down = vmem_call(near_kernel, place, (*shared, low, high), (piece, piece))
    up, down = y_plus(up, 1), y_plus(down, 3)
    small = small + flipped(small, "y", Y, 1)
    small = small + flipped(small, "y", Y, 2)
    (total,) = vmem_call(
        sum_y_kernel, place, (own, up, down, small), (((Z, 400, width), BF),)
    )
    total = exchanged(total, "z")
    blocks, small = vmem_call(
        blocks_kernel, place, (total,), (((X * CORES, 80, width), BF), ((8, width), F32))
    )
    arrived = exchanged(blocks, ("x", "core"))
    (pieces,) = vmem_call(pieces_kernel, place, (arrived,), (((384, width), BF),))
    own = lax.all_gather(pieces, "z")
    below, above = y_plus(own, 1), y_plus(own, 3)
    low, high = y_plus(below[: Z // 2], 1), y_plus(above[Z // 2 :], 3)
    first, second, third = vmem_call(
        out_kernel,
        place,
        (own, below, above, low, high),
        (
            ((X, Y, Z, 32, width), BF),
            ((X, Z, 16, D), BF),
            ((X, CORES, Y, Z, 16, width), BF),
        ),
    )
    return (
        small[1, 0],
        small[1, 1],
        small[0],
        first.reshape(X, D, width),
        second.reshape(X, width, D),
        third.reshape(X, D, width),
    )


def solution(mesh):
    axes = Mesh(mesh.devices.reshape(Z, Y, X, CORES), ("z", "y", "x", "core"))
    batch, dim = ("z", "y"), ("x", "core")
    placed = (
        P(dim),
        P(),
        P(dim),
        P(None, batch, dim),
        P(batch),
        P(dim),
        P(None, None, dim),
        P(None, dim, None),
        P(None, None, dim),
    )
    return jax.shard_map(
        local,
        mesh=axes,
        in_specs=placed,
        out_specs=(
            P(),
            P(),
            P(dim),
            P(None, None, dim),
            P(None, dim, None),
            P(None, None, dim),
        ),
        check_vma=False,
    )
```

```python
import math

import jax
import jax.numpy as jnp
from jax import lax
from jax.experimental import pallas as pl
from jax.experimental.pallas import tpu as pltpu
from jax.sharding import Mesh
from jax.sharding import PartitionSpec as P

D = 1024

DRIFT_RATE = 0.06
VOLATILITY = 0.2
DISCOUNT = 0.02
DEFAULT_LOSS = 1.0 / 3.0

X, CORES, Y, Z = 4, 2, 4, 8
W = D // (X * CORES)
BF = jnp.bfloat16
F32 = jnp.float32


def shifted(value, axis, n, o):
    return lax.ppermute(value, axis, [(i, (i + o) % n) for i in range(n)])


def flipped(value, axis, n, bit):
    return lax.ppermute(value, axis, [(i, i ^ bit) for i in range(n)])


def x_plus(value, o):
    return shifted(value, "x", X, o)


def y_plus(value, o):
    return shifted(value, "y", Y, o)


def z_plus(value, o):
    return shifted(value, "z", Z, o)


def turned(value, r):
    pairs = [(X * y + x, X * ((x + r) % X) + y) for y in range(Y) for x in range(X)]
    return lax.ppermute(value, ("y", "x"), pairs)


def core_swap(value):
    return flipped(value, "core", CORES, 1)


def pick(array, index):
    return lax.dynamic_index_in_dim(array, index, 0, keepdims=False)


def dot(a, b, contract):
    return lax.dot_general(a, b, (contract, ((), ())), preferred_element_type=F32)


def vmem_call(kernel, place, args, outs, scratch=()):
    vmem = pl.BlockSpec(memory_space=pltpu.VMEM)
    return pl.pallas_call(
        kernel,
        out_shape=[jax.ShapeDtypeStruct(shape, dtype) for shape, dtype in outs],
        in_specs=[pl.BlockSpec(memory_space=pltpu.SMEM)] + [vmem] * len(args),
        out_specs=[vmem] * len(outs),
        scratch_shapes=list(scratch),
        name=kernel.__name__,
    )(place, *args)


def two_words(value):
    high = value.astype(BF).astype(F32)
    return jnp.concatenate([high, value - high], axis=0).astype(BF)


def arrange_kernel(place, near, far, inputs, incs):
    x, c, y = place[0], place[1], place[2]
    for i in range(X):
        r = lax.rem(y + (X - i), X)
        inputs[:, pl.ds(pl.multiple_of(2 * W * i + W * c, W), W)] = near[r, 0]
        inputs[:, pl.ds(pl.multiple_of(2 * W * i + W * (1 - c), W), W)] = far[r, 0]
        r = lax.rem(y - x + (X + i), X)
        incs[:, 2 * W * i : 2 * W * i + W] = near[r, 1]
        incs[:, 2 * W * i + W : 2 * W * i + 2 * W] = far[r, 1]


def forward_kernel(place, in_ref, f0, f1, f2, f3, s0, s1, s2, s3, tanh_ref, mine, other, part):
    for o, (first, second) in enumerate(((f0, s0), (f1, s1), (f2, s2), (f3, s3))):
        tanh = jnp.tanh(dot(in_ref[...], first[...], ((1,), (0,))))
        tanh_ref[:, W * o : W * o + W] = tanh
        more = dot(tanh.astype(BF), second[...], ((1,), (0,)))
        part[...] = more if o == 0 else part[...] + more
    half = mine.shape[1]

    @pl.when(place[1] == 0)
    def _():
        mine[...] = part[:, :half]
        other[...] = part[:, half:]

    @pl.when(place[1] != 0)
    def _():
        mine[...] = part[:, half:]
        other[...] = part[:, :half]


def back_kernel(place, inc_ref, n0, n1, n2, n3, f0, f1, f2, f3, out):
    for i, piece in enumerate((n0, f0, n1, f1, n2, f2, n3, f3)):
        more = dot(inc_ref[:, W * i : W * i + W], piece[...], ((1,), (1,)))
        out[...] = more if i == 0 else out[...] + more


def put_sums(outs, o, in_ref, tanh_ref, all_ref, d1_ref, wt_ref, inc_ref, added=None):
    at = slice(W * o, W * o + W)
    g1 = dot(in_ref[...], d1_ref[:, at], ((0,), (0,)))
    g2 = dot(tanh_ref[:, at].astype(BF), all_ref[...], ((0,), (0,)))
    g3 = dot(wt_ref[...], inc_ref[:, 2 * W * o : 2 * W * o + 2 * W], ((0,), (0,)))
    share = Z // len(outs)

    def put(k, row, value):
        rows = value.shape[0]
        if added is not None and k in added[1]:
            value = value + added[0][k - added[1][0], row : row + rows, :].astype(F32)
        outs[k // share][k % share, row : row + rows, :] = value.astype(BF)

    for k in range(Z):
        put(k, 0, g1[W * k : W * k + W])
        put(k, 128, g2[:, W * k : W * k + W])
        put(k, 256, g3[64 * k : 64 * k + 64, :W])
        put(k, 320, g3[64 * k : 64 * k + 64, W:])


def far_kernel(
    place, in_ref, tanh_ref, own_ref, far_ref, s0, s1, s2, s3, wt_ref, inc_ref, low, high, all_ref, d1_ref
):
    half = own_ref.shape[1]

    @pl.when(place[1] == 0)
    def _():
        all_ref[:, :half] = own_ref[...]
        all_ref[:, half:] = far_ref[...]

    @pl.when(place[1] != 0)
    def _():
        all_ref[:, :half] = far_ref[...]
        all_ref[:, half:] = own_ref[...]

    for o, second in enumerate((s0, s1, s2, s3)):
        at = slice(W * o, W * o + W)
        tanh = tanh_ref[:, at]
        back = dot(all_ref[...], second[...], ((1,), (1,)))
        d1_ref[:, at] = (back * (1.0 - tanh * tanh)).astype(BF)
    put_sums((low, high), 2, in_ref, tanh_ref, all_ref, d1_ref, wt_ref, inc_ref)


def own_kernel(place, in_ref, tanh_ref, all_ref, d1_ref, wt_ref, inc_ref, out, token):
    token[...] = jnp.zeros_like(token)
    put_sums((out,), 0, in_ref, tanh_ref, all_ref, d1_ref, wt_ref, inc_ref)


def near_kernel(
    place, in_ref, tanh_ref, all_ref, d1_ref, wt_ref, inc_ref, from_low, from_high, token, small, up, down
):
    rest = (in_ref, tanh_ref, all_ref, d1_ref, wt_ref, inc_ref)
    put_sums((up,), 3, *rest, (from_low, range(Z // 2)))
    put_sums((down,), 1, *rest, (from_high, range(Z // 2, Z)))


def sum_x_kernel(place, own, from_below, from_above, small_ref, *outs):
    rows = own.shape[1]
    small = two_words(small_ref[...])
    for r, out in enumerate(outs):
        k = lax.rem(place[3] + r, Z)
        out[:rows, :] = (
            own[k].astype(F32) + from_below[k].astype(F32) + from_above[k].astype(F32)
        ).astype(BF)
        out[rows:, :] = small


def sum_z_kernel(place, *refs):
    p, out, far = refs[:Z], refs[Z], refs[Z + 1]

    def total(row, rows):
        v = [ref[row : row + rows, :].astype(F32) for ref in p]
        return ((v[0] + v[4]) + (v[2] + v[6])) + ((v[1] + v[5]) + (v[3] + v[7]))

    for row in range(0, 320, 64):
        out[row : row + 64, :] = total(row, 64).astype(BF)
    far[...] = total(320, 64).astype(BF)
    words = total(384, 16)
    out[320:, :] = two_words(words[:8] + words[8:])


def pieces_kernel(place, main, far, out):
    out[:256, :] = main[:256, :]
    c = place[1]
    out[pl.ds(pl.multiple_of(256 + 64 * c, 64), 64), :] = main[256:320, :]
    out[pl.ds(pl.multiple_of(256 + 64 * (1 - c), 64), 64), :] = far[...]
    out[384:, :] = main[320:, :]


def out_kernel(place, own, below, above, low, high, first, second, third, loss, grad_y, grad_z):
    y = place[2]
    parts = [(own, 0, k, k) for k in range(Z)]
    parts += [(below, Y - 1, k, k) for k in range(Z)] + [(above, 1, k, k) for k in range(Z)]
    parts += [(low, 2, k, k) for k in range(Z // 2)]
    parts += [(high, 2, k, k + Z // 2) for k in range(Z // 2)]
    for ref, off, i, k in parts:
        at = lax.rem(y + off, Y)
        first[at, k] = ref[i, :128, :]
        second[at, :, W * k : W * k + W] = ref[i, 128:256, :]
        third[at, 0, k] = ref[i, 256:320, :]
        third[at, 1, k] = ref[i, 320:384, :]

    def words(ref):
        both = ref[0, 384:, :].astype(F32)
        return both[:8] + both[8:]

    small = (words(own) + words(low)) + (words(below) + words(above))
    grad_z[...] = small[0:1, :]
    loss[...] = small[1:2, 0:1]
    grad_y[...] = small[1:2, 1:2]


def factors_of(default_step, steps):
    counter = jnp.arange(steps, dtype=F32)
    factors = (
        1.0
        + DISCOUNT / steps
        - DEFAULT_LOSS * (counter[:, None] == default_step[None, :]).astype(F32)
    )
    coefs = [jnp.ones(default_step.shape, F32)]
    for n in range(steps - 1, 0, -1):
        coefs.append(coefs[-1] * factors[n])
    return factors, jnp.stack(coefs[::-1])


def local(
    x_start, y_start, z_start, increments, default_step, term_weight, w_first, w_second, w_third
):
    steps, paths, width = increments.shape
    tstep = 1.0 / steps
    scale = 1.0 / math.sqrt(paths * Y * Z)
    x, c, y, z = (lax.axis_index(name) for name in ("x", "core", "y", "z"))
    place = jnp.stack([x, c, y, z]).astype(jnp.int32)
    half = D // CORES
    flat = (2, paths // 2)

    states = x_start[None, :] * (1.0 + DRIFT_RATE * tstep + VOLATILITY * increments[0])
    sends = []
    for n in range(1, steps):
        sends.append(jnp.stack([states.astype(BF), increments[n].astype(BF)]))
        states = states * (1.0 + DRIFT_RATE * tstep + VOLATILITY * increments[n])
    sends = jnp.stack(sends)
    near = jnp.stack([turned(pick(sends, (x + r) % X), r) for r in range(X)])
    far = core_swap(near)
    step_here = default_step.astype(F32)
    factors_here, coefs_here = factors_of(step_here, steps)
    target_part = jnp.sum(states * term_weight[None, :], axis=1) / math.sqrt(D)
    first_part = jnp.sum(increments[0] * z_start[None, :], axis=1)
    there = jnp.concatenate(
        [(coefs_here[0] * first_part - target_part).reshape(flat), step_here.reshape(flat)]
    )
    there = turned(there, 0)
    part_sum = there[:2]
    factors, coefs = factors_of(there[2:].reshape(paths), steps)

    def from_row(piece, way):
        below, above = x_plus(piece, 1), x_plus(piece, 3)
        return [piece, below, x_plus(below if way == 1 else above, way), above]

    third = pick(w_third, y).reshape(CORES, half, width)
    far_third = core_swap(pick(third, 1 - c))
    w1 = from_row(pick(w_first, y), 1)
    w2 = from_row(pick(w_second, y), 3)
    w3_near = from_row(pick(third, c), 1)
    w3_far = from_row(far_third, 3)

    inputs, incs = vmem_call(
        arrange_kernel, place, (near, far), (((paths, D), BF), ((paths, D), BF))
    )
    tanh_first, mine, other = vmem_call(
        forward_kernel,
        place,
        (inputs, *w1, *w2),
        [((paths, half), F32)] * 3,
        [pltpu.VMEM((paths, D), F32)],
    )
    other = core_swap(other)
    (back,) = vmem_call(back_kernel, place, (incs, *w3_near, *w3_far), [((paths, half), F32)])
    tanh_second = jnp.tanh(mine + other)
    dots = jnp.sum(tanh_second * back, axis=1)
    coef = pick(coefs, y + 1)
    total = part_sum + (coef * dots).reshape(flat)
    total = total + core_swap(total)
    total = total + flipped(total, "y", Y, 1)
    total = total + flipped(total, "y", Y, 2)
    total = total + (factors[0] * coefs[0] * y_start).reshape(flat)
    adjoint = 2.0 * scale * total.reshape(paths)

    error = turned(total, 0).reshape(paths)
    adjoint_one = 2.0 * scale * error * coefs_here[0]
    loss = scale * jnp.sum(error * error)
    grad_y = jnp.sum(adjoint_one * factors_here[0])
    grad_z = jnp.sum(adjoint_one[:, None] * increments[0], axis=0)
    small = jnp.concatenate(
        [grad_z, jnp.stack([loss, grad_y]), jnp.zeros((7 * width - 2,), F32)]
    ).reshape(8, width)

    weight = (adjoint * coef)[:, None]
    weighted = (weight * tanh_second).astype(BF)
    d_second = (weight * back * (1.0 - tanh_second * tanh_second)).astype(BF)
    d_far = core_swap(d_second)
    low, high, d_all, d_first = vmem_call(
        far_kernel,
        place,
        (inputs, tanh_first, d_second, d_far, *w2, weighted, incs),
        (
            ((Z // 2, 384, width), BF),
            ((Z // 2, 384, width), BF),
            ((paths, D), BF),
            ((paths, half), BF),
        ),
    )
    low, high = x_plus(low, 1), x_plus(high, 3)
    shared = (inputs, tanh_first, d_all, d_first, weighted, incs)
    piece = ((Z, 384, width), BF)
    own, token = vmem_call(own_kernel, place, shared, (piece, ((8, width), F32)))
    up, down = vmem_call(
        near_kernel, place, (*shared, low, high, token, small), (piece, piece)
    )
    up, down = x_plus(up, 1), x_plus(down, 3)
    parts = vmem_call(
        sum_x_kernel, place, (own, up, down, small), [((400, width), BF)] * Z
    )
    parts = [parts[0]] + [z_plus(parts[r], r) for r in range(1, Z)]
    main, far = vmem_call(
        sum_z_kernel, place, parts, (((336, width), BF), ((64, width), BF))
    )
    (pieces,) = vmem_call(pieces_kernel, place, (main, core_swap(far)), (((400, width), BF),))
    own = lax.all_gather(pieces, "z")
    below, above = y_plus(own, 1), y_plus(own, 3)
    low, high = y_plus(below[: Z // 2], 1), y_plus(above[Z // 2 :], 3)
    first, second, third, loss, grad_y, grad_z = vmem_call(
        out_kernel,
        place,
        (own, below, above, low, high),
        (
            ((X, Z, 128, width), BF),
            ((X, 128, D), BF),
            ((X, CORES, Z, 64, width), BF),
            ((1, 1), F32),
            ((1, 1), F32),
            ((1, width), F32),
        ),
    )
    return (
        loss[0, 0],
        grad_y[0, 0],
        grad_z[0],
        first.reshape(X, D, width),
        second,
        third.reshape(X, D, width),
    )


def solution(mesh):
    axes = Mesh(mesh.devices.reshape(Z, Y, X, CORES), ("z", "y", "x", "core"))
    batch, dim = ("z", "y"), ("x", "core")
    placed = (
        P(dim),
        P(),
        P(dim),
        P(None, batch, dim),
        P(batch),
        P(dim),
        P(None, None, dim),
        P(None, dim, None),
        P(None, None, dim),
    )
    return jax.shard_map(
        local,
        mesh=axes,
        in_specs=placed,
        out_specs=(
            P(),
            P(),
            P(dim),
            P(None, None, dim),
            P(None, dim, None),
            P(None, None, dim),
        ),
        check_vma=False,
    )
```

```python
import math

import jax
import jax.numpy as jnp
from jax import lax
from jax.experimental import pallas as pl
from jax.experimental.pallas import tpu as pltpu
from jax.sharding import Mesh
from jax.sharding import PartitionSpec as P

D = 1024

DRIFT_RATE = 0.06
VOLATILITY = 0.2
DISCOUNT = 0.02
DEFAULT_LOSS = 1.0 / 3.0

X, CORES, Y, Z = 4, 2, 4, 8
W = D // (X * CORES)
BF = jnp.bfloat16
F32 = jnp.float32


def shifted(value, axis, n, o):
    return lax.ppermute(value, axis, [(i, (i + o) % n) for i in range(n)])


def flipped(value, axis, n, bit):
    return lax.ppermute(value, axis, [(i, i ^ bit) for i in range(n)])


def x_plus(value, o):
    return shifted(value, "x", X, o)


def y_plus(value, o):
    return shifted(value, "y", Y, o)


def z_plus(value, o):
    return shifted(value, "z", Z, o)


def turned(value, r):
    pairs = [(X * y + x, X * ((x + r) % X) + y) for y in range(Y) for x in range(X)]
    return lax.ppermute(value, ("y", "x"), pairs)


def core_swap(value):
    return flipped(value, "core", CORES, 1)


def pick(array, index):
    return lax.dynamic_index_in_dim(array, index, 0, keepdims=False)


def dot(a, b, contract):
    return lax.dot_general(a, b, (contract, ((), ())), preferred_element_type=F32)


def vmem_call(kernel, place, args, outs, scratch=()):
    vmem = pl.BlockSpec(memory_space=pltpu.VMEM)
    return pl.pallas_call(
        kernel,
        out_shape=[jax.ShapeDtypeStruct(shape, dtype) for shape, dtype in outs],
        in_specs=[pl.BlockSpec(memory_space=pltpu.SMEM)] + [vmem] * len(args),
        out_specs=[vmem] * len(outs),
        scratch_shapes=list(scratch),
        name=kernel.__name__,
    )(place, *args)


def two_words(value):
    high = value.astype(BF).astype(F32)
    return jnp.concatenate([high, value - high], axis=0).astype(BF)


def arrange_kernel(place, near, far, inputs, incs):
    x, c, y = place[0], place[1], place[2]
    for i in range(X):
        r = lax.rem(y + (X - i), X)
        inputs[:, pl.ds(pl.multiple_of(2 * W * i + W * c, W), W)] = near[r, 0]
        inputs[:, pl.ds(pl.multiple_of(2 * W * i + W * (1 - c), W), W)] = far[r, 0]
        r = lax.rem(y - x + (X + i), X)
        incs[:, 2 * W * i : 2 * W * i + W] = near[r, 1]
        incs[:, 2 * W * i + W : 2 * W * i + 2 * W] = far[r, 1]


def pack_kernel(place, first, second, third, far, out, sems):
    c, y = place[1], place[2]
    half = far.shape[0]
    copies = [
        (first.at[y], out.at[:D, :]),
        (third.at[y, c], out.at[2 * D : 2 * D + half, :]),
        (far, out.at[2 * D + half :, :]),
    ]
    for k in range(D // W):
        copies.append((second.at[y, :, pl.ds(W * k, W)], out.at[D + W * k : D + W * k + W, :]))
    copies = [pltpu.make_async_copy(a, b, sems.at[i]) for i, (a, b) in enumerate(copies)]
    for copy in copies:
        copy.start()
    for copy in copies:
        copy.wait()


def rows_of(pieces, row, rows):
    own, below, low, high, above = pieces
    mid = low.shape[0]
    apart = low[row : row + rows, :] if row < mid else high[row - mid : row - mid + rows, :]
    return [own[row : row + rows, :], below[row : row + rows, :], apart, above[row : row + rows, :]]


def forward_kernel(place, in_ref, own, below, low, high, above, tanh_ref, mine, other, part):
    pieces = (own, below, low, high, above)
    for o, first in enumerate(rows_of(pieces, 0, D)):
        tanh_ref[:, W * o : W * o + W] = jnp.tanh(dot(in_ref[...], first, ((1,), (0,))))
    for o in range(X):
        hidden = tanh_ref[:, W * o : W * o + W].astype(BF)
        for k in range(D // W):
            at = slice(W * k, W * k + W)
            more = dot(hidden, rows_of(pieces, D + W * k, W)[o], ((1,), (0,)))
            part[:, at] = more if o == 0 else part[:, at] + more
    half = mine.shape[1]

    @pl.when(place[1] == 0)
    def _():
        mine[...] = part[:, :half]
        other[...] = part[:, half:]

    @pl.when(place[1] != 0)
    def _():
        mine[...] = part[:, half:]
        other[...] = part[:, :half]


def back_kernel(place, inc_ref, own, below, low, high, above, out):
    half = out.shape[1]
    pieces = (own, below, low, high, above)
    for i in range(CORES):
        for o, piece in enumerate(rows_of(pieces, 2 * D + half * i, half)):
            at = W * (CORES * o + i)
            more = dot(inc_ref[:, at : at + W], piece, ((1,), (1,)))
            out[...] = more if i + o == 0 else out[...] + more


def put_sums(outs, o, in_ref, tanh_ref, all_ref, d1_ref, wt_ref, inc_ref, added=None):
    at = slice(W * o, W * o + W)
    g1 = dot(in_ref[...], d1_ref[:, at], ((0,), (0,)))
    g2 = dot(tanh_ref[:, at].astype(BF), all_ref[...], ((0,), (0,)))
    g3 = dot(wt_ref[...], inc_ref[:, 2 * W * o : 2 * W * o + 2 * W], ((0,), (0,)))
    share = Z // len(outs)

    def put(k, row, value):
        rows = value.shape[0]
        if added is not None and k in added[1]:
            value = value + added[0][k - added[1][0], row : row + rows, :].astype(F32)
        outs[k // share][k % share, row : row + rows, :] = value.astype(BF)

    for k in range(Z):
        put(k, 0, g1[W * k : W * k + W])
        put(k, 128, g2[:, W * k : W * k + W])
        put(k, 256, g3[64 * k : 64 * k + 64, :W])
        put(k, 320, g3[64 * k : 64 * k + 64, W:])


def far_kernel(
    place, in_ref, tanh_ref, own_ref, far_ref, own, below, w_low, w_high, above, wt_ref, inc_ref,
    low, high, all_ref, d1_ref, back_ref
):
    half = own_ref.shape[1]

    @pl.when(place[1] == 0)
    def _():
        all_ref[:, :half] = own_ref[...]
        all_ref[:, half:] = far_ref[...]

    @pl.when(place[1] != 0)
    def _():
        all_ref[:, :half] = far_ref[...]
        all_ref[:, half:] = own_ref[...]

    pieces = (own, below, w_low, w_high, above)
    for o in range(X):
        at = slice(W * o, W * o + W)
        for k in range(D // W):
            d_second = all_ref[:, W * k : W * k + W]
            more = dot(d_second, rows_of(pieces, D + W * k, W)[o], ((1,), (1,)))
            back_ref[...] = more if k == 0 else back_ref[...] + more
        tanh = tanh_ref[:, at]
        d1_ref[:, at] = (back_ref[...] * (1.0 - tanh * tanh)).astype(BF)
    put_sums((low, high), 2, in_ref, tanh_ref, all_ref, d1_ref, wt_ref, inc_ref)


def own_kernel(place, in_ref, tanh_ref, all_ref, d1_ref, wt_ref, inc_ref, out, token):
    token[...] = jnp.zeros_like(token)
    put_sums((out,), 0, in_ref, tanh_ref, all_ref, d1_ref, wt_ref, inc_ref)


def near_kernel(
    place, in_ref, tanh_ref, all_ref, d1_ref, wt_ref, inc_ref, from_low, from_high, token, small, up, down
):
    rest = (in_ref, tanh_ref, all_ref, d1_ref, wt_ref, inc_ref)
    put_sums((up,), 3, *rest, (from_low, range(Z // 2)))
    put_sums((down,), 1, *rest, (from_high, range(Z // 2, Z)))


def sum_x_kernel(place, own, from_below, from_above, small_ref, *outs):
    rows = own.shape[1]
    small = two_words(small_ref[...])
    for r, out in enumerate(outs):
        k = lax.rem(place[3] + r, Z)
        out[:rows, :] = (
            own[k].astype(F32) + from_below[k].astype(F32) + from_above[k].astype(F32)
        ).astype(BF)
        out[rows:, :] = small


def sum_z_kernel(place, *refs):
    p, out, far = refs[:Z], refs[Z], refs[Z + 1]

    def total(row, rows):
        v = [ref[row : row + rows, :].astype(F32) for ref in p]
        return ((v[0] + v[4]) + (v[2] + v[6])) + ((v[1] + v[5]) + (v[3] + v[7]))

    for row in range(0, 320, 64):
        out[row : row + 64, :] = total(row, 64).astype(BF)
    far[...] = total(320, 64).astype(BF)
    words = total(384, 16)
    out[320:, :] = two_words(words[:8] + words[8:])


def pieces_kernel(place, main, far, out):
    out[:256, :] = main[:256, :]
    c = place[1]
    out[pl.ds(pl.multiple_of(256 + 64 * c, 64), 64), :] = main[256:320, :]
    out[pl.ds(pl.multiple_of(256 + 64 * (1 - c), 64), 64), :] = far[...]
    out[384:, :] = main[320:, :]


def out_kernel(place, own, below, above, low, high, first, second, third, loss, grad_y, grad_z):
    y = place[2]
    parts = [(own, 0, k, k) for k in range(Z)]
    parts += [(below, Y - 1, k, k) for k in range(Z)] + [(above, 1, k, k) for k in range(Z)]
    parts += [(low, 2, k, k) for k in range(Z // 2)]
    parts += [(high, 2, k, k + Z // 2) for k in range(Z // 2)]
    for ref, off, i, k in parts:
        at = lax.rem(y + off, Y)
        first[at, k] = ref[i, :128, :]
        second[at, :, W * k : W * k + W] = ref[i, 128:256, :]
        third[at, 0, k] = ref[i, 256:320, :]
        third[at, 1, k] = ref[i, 320:384, :]

    def words(ref):
        both = ref[0, 384:, :].astype(F32)
        return both[:8] + both[8:]

    small = (words(own) + words(low)) + (words(below) + words(above))
    grad_z[...] = small[0:1, :]
    loss[...] = small[1:2, 0:1]
    grad_y[...] = small[1:2, 1:2]


def factors_of(default_step, steps):
    counter = jnp.arange(steps, dtype=F32)
    factors = (
        1.0
        + DISCOUNT / steps
        - DEFAULT_LOSS * (counter[:, None] == default_step[None, :]).astype(F32)
    )
    coefs = [jnp.ones(default_step.shape, F32)]
    for n in range(steps - 1, 0, -1):
        coefs.append(coefs[-1] * factors[n])
    return factors, jnp.stack(coefs[::-1])


def local(
    x_start, y_start, z_start, increments, default_step, term_weight, w_first, w_second, w_third
):
    steps, paths, width = increments.shape
    tstep = 1.0 / steps
    scale = 1.0 / math.sqrt(paths * Y * Z)
    x, c, y, z = (lax.axis_index(name) for name in ("x", "core", "y", "z"))
    place = jnp.stack([x, c, y, z]).astype(jnp.int32)
    half = D // CORES
    flat = (2, paths // 2)

    states = x_start[None, :] * (1.0 + DRIFT_RATE * tstep + VOLATILITY * increments[0])
    sends = []
    for n in range(1, steps):
        sends.append(jnp.stack([states.astype(BF), increments[n].astype(BF)]))
        states = states * (1.0 + DRIFT_RATE * tstep + VOLATILITY * increments[n])
    sends = jnp.stack(sends)
    near = jnp.stack([turned(pick(sends, (x + r) % X), r) for r in range(X)])
    far = core_swap(near)
    step_here = default_step.astype(F32)
    factors_here, coefs_here = factors_of(step_here, steps)
    target_part = jnp.sum(states * term_weight[None, :], axis=1) / math.sqrt(D)
    first_part = jnp.sum(increments[0] * z_start[None, :], axis=1)
    there = jnp.concatenate(
        [(coefs_here[0] * first_part - target_part).reshape(flat), step_here.reshape(flat)]
    )
    there = turned(there, 0)
    part_sum = there[:2]
    factors, coefs = factors_of(there[2:].reshape(paths), steps)

    third = w_third.reshape(X, CORES, half, width)
    far_third = core_swap(lax.dynamic_slice(third, (y, 1 - c, 0, 0), (1, 1, half, width))[0, 0])
    anywhere = pl.BlockSpec(memory_space=pl.ANY)
    packed = pl.pallas_call(
        pack_kernel,
        out_shape=jax.ShapeDtypeStruct((3 * D, width), BF),
        in_specs=[pl.BlockSpec(memory_space=pltpu.SMEM)] + [anywhere] * 4,
        out_specs=pl.BlockSpec(memory_space=pltpu.VMEM),
        scratch_shapes=[pltpu.SemaphoreType.DMA((3 + D // W,))],
        name="pack_kernel",
    )(place, w_first, w_second, third, far_third)
    below, above = x_plus(packed, 1), x_plus(packed, 3)
    mid = 3 * D // 2
    weights = (packed, below, x_plus(below[:mid], 1), x_plus(above[mid:], 3), above)

    inputs, incs = vmem_call(
        arrange_kernel, place, (near, far), (((paths, D), BF), ((paths, D), BF))
    )
    tanh_first, mine, other = vmem_call(
        forward_kernel,
        place,
        (inputs, *weights),
        [((paths, half), F32)] * 3,
        [pltpu.VMEM((paths, D), F32)],
    )
    other = core_swap(other)
    (back,) = vmem_call(back_kernel, place, (incs, *weights), [((paths, half), F32)])
    tanh_second = jnp.tanh(mine + other)
    dots = jnp.sum(tanh_second * back, axis=1)
    coef = pick(coefs, y + 1)
    total = part_sum + (coef * dots).reshape(flat)
    total = total + core_swap(total)
    total = total + flipped(total, "y", Y, 1)
    total = total + flipped(total, "y", Y, 2)
    total = total + (factors[0] * coefs[0] * y_start).reshape(flat)
    adjoint = 2.0 * scale * total.reshape(paths)

    error = turned(total, 0).reshape(paths)
    adjoint_one = 2.0 * scale * error * coefs_here[0]
    loss = scale * jnp.sum(error * error)
    grad_y = jnp.sum(adjoint_one * factors_here[0])
    grad_z = jnp.sum(adjoint_one[:, None] * increments[0], axis=0)
    small = jnp.concatenate(
        [grad_z, jnp.stack([loss, grad_y]), jnp.zeros((7 * width - 2,), F32)]
    ).reshape(8, width)

    weight = (adjoint * coef)[:, None]
    weighted = (weight * tanh_second).astype(BF)
    d_second = (weight * back * (1.0 - tanh_second * tanh_second)).astype(BF)
    d_far = core_swap(d_second)
    low, high, d_all, d_first = vmem_call(
        far_kernel,
        place,
        (inputs, tanh_first, d_second, d_far, *weights, weighted, incs),
        (
            ((Z // 2, 384, width), BF),
            ((Z // 2, 384, width), BF),
            ((paths, D), BF),
            ((paths, half), BF),
        ),
        [pltpu.VMEM((paths, width), F32)],
    )
    low, high = x_plus(low, 1), x_plus(high, 3)
    shared = (inputs, tanh_first, d_all, d_first, weighted, incs)
    piece = ((Z, 384, width), BF)
    own, token = vmem_call(own_kernel, place, shared, (piece, ((8, width), F32)))
    up, down = vmem_call(
        near_kernel, place, (*shared, low, high, token, small), (piece, piece)
    )
    up, down = x_plus(up, 1), x_plus(down, 3)
    parts = vmem_call(
        sum_x_kernel, place, (own, up, down, small), [((400, width), BF)] * Z
    )
    parts = [parts[0]] + [z_plus(parts[r], r) for r in range(1, Z)]
    main, far = vmem_call(
        sum_z_kernel, place, parts, (((336, width), BF), ((64, width), BF))
    )
    (pieces,) = vmem_call(pieces_kernel, place, (main, core_swap(far)), (((400, width), BF),))
    own = lax.all_gather(pieces, "z")
    below, above = y_plus(own, 1), y_plus(own, 3)
    low, high = y_plus(below[: Z // 2], 1), y_plus(above[Z // 2 :], 3)
    first, second, third, loss, grad_y, grad_z = vmem_call(
        out_kernel,
        place,
        (own, below, above, low, high),
        (
            ((X, Z, 128, width), BF),
            ((X, 128, D), BF),
            ((X, CORES, Z, 64, width), BF),
            ((1, 1), F32),
            ((1, 1), F32),
            ((1, width), F32),
        ),
    )
    return (
        loss[0, 0],
        grad_y[0, 0],
        grad_z[0],
        first.reshape(X, D, width),
        second,
        third.reshape(X, D, width),
    )


def solution(mesh):
    axes = Mesh(mesh.devices.reshape(Z, Y, X, CORES), ("z", "y", "x", "core"))
    batch, dim = ("z", "y"), ("x", "core")
    placed = (
        P(dim),
        P(),
        P(dim),
        P(None, batch, dim),
        P(batch),
        P(dim),
        P(None, None, dim),
        P(None, dim, None),
        P(None, None, dim),
    )
    return jax.shard_map(
        local,
        mesh=axes,
        in_specs=placed,
        out_specs=(
            P(),
            P(),
            P(dim),
            P(None, None, dim),
            P(None, dim, None),
            P(None, None, dim),
        ),
        check_vma=False,
    )
```

```python
import math

import jax
import jax.numpy as jnp
from jax import lax
from jax.experimental import pallas as pl
from jax.experimental.pallas import tpu as pltpu
from jax.sharding import Mesh
from jax.sharding import PartitionSpec as P


D = 1024

DRIFT_RATE = 0.06
VOLATILITY = 0.2
DISCOUNT = 0.02
DEFAULT_LOSS = 1.0 / 3.0

X, CORES, Y, Z = 4, 2, 4, 8
W = D // (X * CORES)
BF = jnp.bfloat16
F32 = jnp.float32


def shifted(value, axis, n, o):
    return lax.ppermute(value, axis, [(i, (i + o) % n) for i in range(n)])


def flipped(value, axis, n, bit):
    return lax.ppermute(value, axis, [(i, i ^ bit) for i in range(n)])


def x_plus(value, o):
    return shifted(value, "x", X, o)


def y_plus(value, o):
    return shifted(value, "y", Y, o)


def z_plus(value, o):
    return shifted(value, "z", Z, o)


def turned(value):
    pairs = [(X * y + x, X * x + y) for y in range(Y) for x in range(X)]
    return lax.ppermute(value, ("y", "x"), pairs)


def core_swap(value):
    return flipped(value, "core", CORES, 1)


def pick(array, index):
    return lax.dynamic_index_in_dim(array, index, 0, keepdims=False)


def dot(a, b, contract):
    return lax.dot_general(a, b, (contract, ((), ())), preferred_element_type=F32)


def vmem_call(kernel, place, args, outs, scratch=()):
    vmem = pl.BlockSpec(memory_space=pltpu.VMEM)
    return pl.pallas_call(
        kernel,
        out_shape=[jax.ShapeDtypeStruct(shape, dtype) for shape, dtype in outs],
        in_specs=[pl.BlockSpec(memory_space=pltpu.SMEM)] + [vmem] * len(args),
        out_specs=[vmem] * len(outs),
        scratch_shapes=list(scratch),
    )(place, *args)


def two_words(value):
    high = value.astype(BF).astype(F32)
    return jnp.concatenate([high, value - high], axis=0).astype(BF)


def arrange_kernel(place, near, far, inputs, incs):
    x, c = place[0], place[1]
    for i in range(X):
        r = lax.rem(x + (X - i), X)
        inputs[:, pl.ds(pl.multiple_of(2 * W * i + W * c, W), W)] = near[r, 0]
        inputs[:, pl.ds(pl.multiple_of(2 * W * i + W * (1 - c), W), W)] = far[r, 0]
        incs[:, 2 * W * i : 2 * W * i + W] = near[i, 1]
        incs[:, 2 * W * i + W : 2 * W * i + 2 * W] = far[i, 1]


def pack_kernel(place, first, second, third, far, out, sems):
    c, y = place[1], place[2]
    half = far.shape[0]
    copies = [
        (first.at[y], out.at[:D, :]),
        (third.at[y, c], out.at[2 * D : 2 * D + half, :]),
        (far, out.at[2 * D + half :, :]),
    ]
    for k in range(D // W):
        copies.append((second.at[y, :, pl.ds(W * k, W)], out.at[D + W * k : D + W * k + W, :]))
    copies = [pltpu.make_async_copy(a, b, sems.at[i]) for i, (a, b) in enumerate(copies)]
    for copy in copies:
        copy.start()
    for copy in copies:
        copy.wait()


def rows_of(pieces, row, rows):
    own, below, low, high, above = pieces
    mid = low.shape[0]
    apart = low[row : row + rows, :] if row < mid else high[row - mid : row - mid + rows, :]
    return [own[row : row + rows, :], below[row : row + rows, :], apart, above[row : row + rows, :]]


def forward_kernel(place, in_ref, own, below, low, high, above, tanh_ref, mine, other, part):
    pieces = (own, below, low, high, above)
    for o, first in enumerate(rows_of(pieces, 0, D)):
        tanh_ref[:, W * o : W * o + W] = jnp.tanh(dot(in_ref[...], first, ((1,), (0,))))
    for o in range(X):
        hidden = tanh_ref[:, W * o : W * o + W].astype(BF)
        for k in range(D // W):
            at = slice(W * k, W * k + W)
            more = dot(hidden, rows_of(pieces, D + W * k, W)[o], ((1,), (0,)))
            part[:, at] = more if o == 0 else part[:, at] + more
    half = mine.shape[1]

    @pl.when(place[1] == 0)
    def _():
        mine[...] = part[:, :half]
        other[...] = part[:, half:]

    @pl.when(place[1] != 0)
    def _():
        mine[...] = part[:, half:]
        other[...] = part[:, :half]


def back_kernel(place, inc_ref, own, below, low, high, above, out):
    half = out.shape[1]
    pieces = (own, below, low, high, above)
    for i in range(CORES):
        for o, piece in enumerate(rows_of(pieces, 2 * D + half * i, half)):
            at = W * (CORES * o + i)
            more = dot(inc_ref[:, at : at + W], piece, ((1,), (1,)))
            out[...] = more if i + o == 0 else out[...] + more


def put_sums(outs, o, in_ref, tanh_ref, all_ref, d1_ref, wt_ref, inc_ref, added=None):
    at = slice(W * o, W * o + W)
    g1 = dot(in_ref[...], d1_ref[:, at], ((0,), (0,)))
    g2 = dot(tanh_ref[:, at].astype(BF), all_ref[...], ((0,), (0,)))
    g3 = dot(wt_ref[...], inc_ref[:, 2 * W * o : 2 * W * o + 2 * W], ((0,), (0,)))
    share = Z // len(outs)

    def put(k, row, value):
        rows = value.shape[0]
        if added is not None and k in added[1]:
            value = value + added[0][k - added[1][0], row : row + rows, :].astype(F32)
        outs[k // share][k % share, row : row + rows, :] = value.astype(BF)

    for k in range(Z):
        put(k, 0, g1[W * k : W * k + W])
        put(k, 128, g2[:, W * k : W * k + W])
        put(k, 256, g3[64 * k : 64 * k + 64, :W])
        put(k, 320, g3[64 * k : 64 * k + 64, W:])


def far_kernel(
    place, in_ref, tanh_ref, own_ref, far_ref, own, below, w_low, w_high, above, wt_ref, inc_ref,
    error, low, high, all_ref, d1_ref, sent, back_ref
):
    sent[...] = error[...]
    half = own_ref.shape[1]

    @pl.when(place[1] == 0)
    def _():
        all_ref[:, :half] = own_ref[...]
        all_ref[:, half:] = far_ref[...]

    @pl.when(place[1] != 0)
    def _():
        all_ref[:, :half] = far_ref[...]
        all_ref[:, half:] = own_ref[...]

    pieces = (own, below, w_low, w_high, above)
    for o in range(X):
        at = slice(W * o, W * o + W)
        for k in range(D // W):
            d_second = all_ref[:, W * k : W * k + W]
            more = dot(d_second, rows_of(pieces, D + W * k, W)[o], ((1,), (1,)))
            back_ref[...] = more if k == 0 else back_ref[...] + more
        tanh = tanh_ref[:, at]
        d1_ref[:, at] = (back_ref[...] * (1.0 - tanh * tanh)).astype(BF)
    put_sums((low, high), 2, in_ref, tanh_ref, all_ref, d1_ref, wt_ref, inc_ref)


def own_kernel(place, in_ref, tanh_ref, all_ref, d1_ref, wt_ref, inc_ref, out, token):
    token[...] = jnp.zeros_like(token)
    put_sums((out,), 0, in_ref, tanh_ref, all_ref, d1_ref, wt_ref, inc_ref)


def near_kernel(
    place, in_ref, tanh_ref, all_ref, d1_ref, wt_ref, inc_ref, from_low, from_high, token, small, up, down
):
    rest = (in_ref, tanh_ref, all_ref, d1_ref, wt_ref, inc_ref)
    put_sums((up,), 3, *rest, (from_low, range(Z // 2)))
    put_sums((down,), 1, *rest, (from_high, range(Z // 2, Z)))


def sum_x_kernel(place, own, from_below, from_above, small_ref, *outs):
    rows = own.shape[1]
    small = two_words(small_ref[...])
    for r, out in enumerate(outs):
        k = lax.rem(place[3] + r, Z)
        out[:rows, :] = (
            own[k].astype(F32) + from_below[k].astype(F32) + from_above[k].astype(F32)
        ).astype(BF)
        out[rows:, :] = small


def sum_z_kernel(place, *refs):
    p, out, far = refs[:Z], refs[Z], refs[Z + 1]

    def total(row, rows):
        v = [ref[row : row + rows, :].astype(F32) for ref in p]
        return ((v[0] + v[4]) + (v[2] + v[6])) + ((v[1] + v[5]) + (v[3] + v[7]))

    for row in range(0, 320, 64):
        out[row : row + 64, :] = total(row, 64).astype(BF)
    far[...] = total(320, 64).astype(BF)
    words = total(384, 16)
    out[320:, :] = two_words(words[:8] + words[8:])


def pieces_kernel(place, main, far, out):
    out[:256, :] = main[:256, :]
    c = place[1]
    out[pl.ds(pl.multiple_of(256 + 64 * c, 64), 64), :] = main[256:320, :]
    out[pl.ds(pl.multiple_of(256 + 64 * (1 - c), 64), 64), :] = far[...]
    out[384:, :] = main[320:, :]


def out_kernel(place, own, below, above, low, high, first, second, third, loss, grad_y, grad_z):
    y = place[2]
    parts = [(own, 0, k, k) for k in range(Z)]
    parts += [(below, Y - 1, k, k) for k in range(Z)] + [(above, 1, k, k) for k in range(Z)]
    parts += [(low, 2, k, k) for k in range(Z // 2)]
    parts += [(high, 2, k, k + Z // 2) for k in range(Z // 2)]
    for ref, off, i, k in parts:
        at = lax.rem(y + off, Y)
        first[at, k] = ref[i, :128, :]
        second[at, :, W * k : W * k + W] = ref[i, 128:256, :]
        third[at, 0, k] = ref[i, 256:320, :]
        third[at, 1, k] = ref[i, 320:384, :]

    def words(ref):
        both = ref[0, 384:, :].astype(F32)
        return both[:8] + both[8:]

    small = (words(own) + words(low)) + (words(below) + words(above))
    grad_z[...] = small[0:1, :]
    loss[...] = small[1:2, 0:1]
    grad_y[...] = small[1:2, 1:2]


def factors_of(default_step, steps):
    counter = jnp.arange(steps, dtype=F32)
    factors = (
        1.0
        + DISCOUNT / steps
        - DEFAULT_LOSS * (counter[:, None] == default_step[None, :]).astype(F32)
    )
    coefs = [jnp.ones(default_step.shape, F32)]
    for n in range(steps - 1, 0, -1):
        coefs.append(coefs[-1] * factors[n])
    return factors, jnp.stack(coefs[::-1])


def local(
    x_start, y_start, z_start, increments, default_step, term_weight, w_first, w_second, w_third
):
    steps, paths, width = increments.shape
    tstep = 1.0 / steps
    scale = 1.0 / math.sqrt(paths * Y * Z)
    x, c, y, z = (lax.axis_index(name) for name in ("x", "core", "y", "z"))
    place = jnp.stack([x, c, y, z]).astype(jnp.int32)
    half = D // CORES
    flat = (2, paths // 2)

    third = w_third.reshape(X, CORES, half, width)
    far_third = core_swap(lax.dynamic_slice(third, (y, 1 - c, 0, 0), (1, 1, half, width))[0, 0])
    anywhere = pl.BlockSpec(memory_space=pl.ANY)
    packed = pl.pallas_call(
        pack_kernel,
        out_shape=jax.ShapeDtypeStruct((3 * D, width), BF),
        in_specs=[pl.BlockSpec(memory_space=pltpu.SMEM)] + [anywhere] * 4,
        out_specs=pl.BlockSpec(memory_space=pltpu.VMEM),
        scratch_shapes=[pltpu.SemaphoreType.DMA((3 + D // W,))],
        name="pack_kernel",
    )(place, w_first, w_second, third, far_third)
    increments, packed = lax.optimization_barrier((increments, packed))

    states = x_start[None, :] * (1.0 + DRIFT_RATE * tstep + VOLATILITY * increments[0])
    sends = []
    for n in range(1, steps):
        sends.append(jnp.stack([states.astype(BF), increments[n].astype(BF)]))
        states = states * (1.0 + DRIFT_RATE * tstep + VOLATILITY * increments[n])
    sends = jnp.stack(sends)
    rows = [pick(sends, y)] + [y_plus(pick(sends, (y + r) % Y), r) for r in range(1, Y)]
    rows = jnp.stack(rows)
    near = [pick(rows, (y - x + X) % X)]
    near += [x_plus(pick(rows, (y - x - q + 2 * X) % X), q) for q in range(1, X)]
    below, above = x_plus(packed, 1), x_plus(packed, 3)
    near, _, _ = lax.optimization_barrier((near, below, above))
    mid = 3 * D // 2
    low = x_plus(below[:mid], 1)
    high = x_plus(above[mid:], 3)
    weights = (packed, below, low, high, above)
    near = jnp.stack(near)
    far = core_swap(near)
    step_here = default_step.astype(F32)
    factors_here, coefs_here = factors_of(step_here, steps)
    target_part = jnp.sum(states * term_weight[None, :], axis=1) / math.sqrt(D)
    first_part = jnp.sum(increments[0] * z_start[None, :], axis=1)
    there = jnp.concatenate(
        [(coefs_here[0] * first_part - target_part).reshape(flat), step_here.reshape(flat)]
    )
    there = turned(there)
    part_sum = there[:2]
    factors, coefs = factors_of(there[2:].reshape(paths), steps)

    inputs, incs = vmem_call(
        arrange_kernel, place, (near, far), (((paths, D), BF), ((paths, D), BF))
    )
    tanh_first, mine, other = vmem_call(
        forward_kernel,
        place,
        (inputs, *weights),
        [((paths, half), F32)] * 3,
        [pltpu.VMEM((paths, D), F32)],
    )
    other = core_swap(other)
    (back,) = vmem_call(back_kernel, place, (incs, *weights), [((paths, half), F32)])
    tanh_second = jnp.tanh(mine + other)
    dots = jnp.sum(tanh_second * back, axis=1)
    coef = pick(coefs, y + 1)
    total = part_sum + (coef * dots).reshape(flat)
    total = total + core_swap(total)
    others = [y_plus(total, r) for r in range(1, Y)]
    total = (total + others[1]) + (others[0] + others[2])
    total = total + (factors[0] * coefs[0] * y_start).reshape(flat)
    adjoint = 2.0 * scale * total.reshape(paths)

    weight = (adjoint * coef)[:, None]
    weighted = (weight * tanh_second).astype(BF)
    d_second = (weight * back * (1.0 - tanh_second * tanh_second)).astype(BF)
    d_far = core_swap(d_second)
    low, high, d_all, d_first, sent = vmem_call(
        far_kernel,
        place,
        (inputs, tanh_first, d_second, d_far, *weights, weighted, incs, total),
        (
            ((Z // 2, 384, width), BF),
            ((Z // 2, 384, width), BF),
            ((paths, D), BF),
            ((paths, half), BF),
            (flat, F32),
        ),
        [pltpu.VMEM((paths, width), F32)],
    )
    error = turned(sent).reshape(paths)
    adjoint_one = 2.0 * scale * error * coefs_here[0]
    loss = scale * jnp.sum(error * error)
    grad_y = jnp.sum(adjoint_one * factors_here[0])
    grad_z = jnp.sum(adjoint_one[:, None] * increments[0], axis=0)
    small = jnp.concatenate(
        [grad_z, jnp.stack([loss, grad_y]), jnp.zeros((7 * width - 2,), F32)]
    ).reshape(8, width)

    low, high = x_plus(low, 1), x_plus(high, 3)
    shared = (inputs, tanh_first, d_all, d_first, weighted, incs)
    piece = ((Z, 384, width), BF)
    own, token = vmem_call(own_kernel, place, shared, (piece, ((8, width), F32)))
    up, down = vmem_call(
        near_kernel, place, (*shared, low, high, token, small), (piece, piece)
    )
    up, down = x_plus(up, 1), x_plus(down, 3)
    parts = vmem_call(
        sum_x_kernel, place, (own, up, down, small), [((400, width), BF)] * Z
    )
    parts = [parts[0]] + [z_plus(parts[r], r) for r in range(1, Z)]
    main, far = vmem_call(
        sum_z_kernel, place, parts, (((336, width), BF), ((64, width), BF))
    )
    (pieces,) = vmem_call(pieces_kernel, place, (main, core_swap(far)), (((400, width), BF),))
    own = lax.all_gather(pieces, "z")
    below, above = y_plus(own, 1), y_plus(own, 3)
    low, high = y_plus(below[: Z // 2], 1), y_plus(above[Z // 2 :], 3)
    first, second, third, loss, grad_y, grad_z = vmem_call(
        out_kernel,
        place,
        (own, below, above, low, high),
        (
            ((X, Z, 128, width), BF),
            ((X, 128, D), BF),
            ((X, CORES, Z, 64, width), BF),
            ((1, 1), F32),
            ((1, 1), F32),
            ((1, width), F32),
        ),
    )
    return (
        loss[0, 0],
        grad_y[0, 0],
        grad_z[0],
        first.reshape(X, D, width),
        second,
        third.reshape(X, D, width),
    )


def solution(mesh):
    axes = Mesh(mesh.devices.reshape(Z, Y, X, CORES), ("z", "y", "x", "core"))
    batch, dim = ("z", "y"), ("x", "core")
    placed = (
        P(dim),
        P(),
        P(dim),
        P(None, batch, dim),
        P(batch),
        P(dim),
        P(None, None, dim),
        P(None, dim, None),
        P(None, None, dim),
    )

    return jax.shard_map(
        local,
        mesh=axes,
        in_specs=placed,
        out_specs=(
            P(),
            P(),
            P(dim),
            P(None, None, dim),
            P(None, dim, None),
            P(None, None, dim),
        ),
        check_vma=False,
    )
```

```python
import math

import jax
import jax.numpy as jnp
from jax import lax
from jax.experimental import pallas as pl
from jax.experimental.pallas import tpu as pltpu
from jax.sharding import Mesh
from jax.sharding import PartitionSpec as P


D = 1024

DRIFT_RATE = 0.06
VOLATILITY = 0.2
DISCOUNT = 0.02
DEFAULT_LOSS = 1.0 / 3.0

X, CORES, Y, Z = 4, 2, 4, 8
W = D // (X * CORES)
ROOM = 20 << 20
BF = jnp.bfloat16
F32 = jnp.float32


def shifted(value, axis, n, o):
    return lax.ppermute(value, axis, [(i, (i + o) % n) for i in range(n)])


def flipped(value, axis, n, bit):
    return lax.ppermute(value, axis, [(i, i ^ bit) for i in range(n)])


def x_plus(value, o):
    return shifted(value, "x", X, o)


def y_plus(value, o):
    return shifted(value, "y", Y, o)


def z_plus(value, o):
    return shifted(value, "z", Z, o)


def turned(value):
    pairs = [(X * y + x, X * x + y) for y in range(Y) for x in range(X)]
    return lax.ppermute(value, ("y", "x"), pairs)


def core_swap(value):
    return flipped(value, "core", CORES, 1)


def pick(array, index):
    return lax.dynamic_index_in_dim(array, index, 0, keepdims=False)


def dot(a, b, contract):
    return lax.dot_general(a, b, (contract, ((), ())), preferred_element_type=F32)


def vmem_call(kernel, place, args, outs, scratch=()):
    vmem = pl.BlockSpec(memory_space=pltpu.VMEM)
    return pl.pallas_call(
        kernel,
        out_shape=[jax.ShapeDtypeStruct(shape, dtype) for shape, dtype in outs],
        in_specs=[pl.BlockSpec(memory_space=pltpu.SMEM)] + [vmem] * len(args),
        out_specs=[vmem] * len(outs),
        scratch_shapes=list(scratch),
        compiler_params=pltpu.CompilerParams(vmem_limit_bytes=ROOM),
    )(place, *args)


def two_words(value):
    high = value.astype(BF).astype(F32)
    return jnp.concatenate([high, value - high], axis=0).astype(BF)


def arrange_kernel(place, near, far, inputs, incs):
    x, c = place[0], place[1]
    for i in range(X):
        r = lax.rem(x + (X - i), X)
        inputs[:, pl.ds(pl.multiple_of(2 * W * i + W * c, W), W)] = near[r, 0]
        inputs[:, pl.ds(pl.multiple_of(2 * W * i + W * (1 - c), W), W)] = far[r, 0]
        incs[:, 2 * W * i : 2 * W * i + W] = near[i, 1]
        incs[:, 2 * W * i + W : 2 * W * i + 2 * W] = far[i, 1]


def pack_kernel(place, first, second, third, far, out, sems):
    c, y = place[1], place[2]
    half = far.shape[0]
    copies = [
        (first.at[y], out.at[:D, :]),
        (third.at[y, c], out.at[2 * D : 2 * D + half, :]),
    ]
    for k in range(D // W):
        copies.append((second.at[y, :, pl.ds(W * k, W)], out.at[D + W * k : D + W * k + W, :]))
    copies = [pltpu.make_async_copy(a, b, sems.at[i]) for i, (a, b) in enumerate(copies)]
    for copy in copies:
        copy.start()
    out[2 * D + half :, :] = far[...]
    for copy in copies:
        copy.wait()


def rows_of(pieces, row, rows):
    own, below, low, high, above = pieces
    mid = low.shape[0]
    apart = low[row : row + rows, :] if row < mid else high[row - mid : row - mid + rows, :]
    return [own[row : row + rows, :], below[row : row + rows, :], apart, above[row : row + rows, :]]


def forward_kernel(place, in_ref, own, below, low, high, above, tanh_ref, mine, other, part):
    pieces = (own, below, low, high, above)
    for o, first in enumerate(rows_of(pieces, 0, D)):
        tanh_ref[:, W * o : W * o + W] = jnp.tanh(dot(in_ref[...], first, ((1,), (0,))))
    for o in range(X):
        hidden = tanh_ref[:, W * o : W * o + W].astype(BF)
        for k in range(D // W):
            at = slice(W * k, W * k + W)
            more = dot(hidden, rows_of(pieces, D + W * k, W)[o], ((1,), (0,)))
            part[:, at] = more if o == 0 else part[:, at] + more
    half = mine.shape[1]

    @pl.when(place[1] == 0)
    def _():
        mine[...] = part[:, :half]
        other[...] = part[:, half:]

    @pl.when(place[1] != 0)
    def _():
        mine[...] = part[:, half:]
        other[...] = part[:, :half]


def back_kernel(place, inc_ref, own, below, low, high, above, out):
    half = out.shape[1]
    pieces = (own, below, low, high, above)
    for i in range(CORES):
        for o, piece in enumerate(rows_of(pieces, 2 * D + half * i, half)):
            at = W * (CORES * o + i)
            more = dot(inc_ref[:, at : at + W], piece, ((1,), (1,)))
            out[...] = more if i + o == 0 else out[...] + more


def put_sums(outs, o, in_ref, tanh_ref, all_ref, d1_ref, wt_ref, inc_ref, added=None):
    at = slice(W * o, W * o + W)
    g1 = dot(in_ref[...], d1_ref[:, at], ((0,), (0,)))
    g2 = dot(tanh_ref[:, at].astype(BF), all_ref[...], ((0,), (0,)))
    g3 = dot(wt_ref[...], inc_ref[:, 2 * W * o : 2 * W * o + 2 * W], ((0,), (0,)))
    share = Z // len(outs)

    def put(k, row, value):
        rows = value.shape[0]
        if added is not None and k in added[1]:
            value = value + added[0][k - added[1][0], row : row + rows, :].astype(F32)
        outs[k // share][k % share, row : row + rows, :] = value.astype(BF)

    for k in range(Z):
        put(k, 0, g1[W * k : W * k + W])
        put(k, 128, g2[:, W * k : W * k + W])
        put(k, 256, g3[64 * k : 64 * k + 64, :W])
        put(k, 320, g3[64 * k : 64 * k + 64, W:])


def far_kernel(
    place, in_ref, tanh_ref, own_ref, far_ref, own, below, w_low, w_high, above, wt_ref, inc_ref,
    error, low, high, all_ref, d1_ref, sent, back_ref
):
    sent[...] = error[...]
    half = own_ref.shape[1]

    @pl.when(place[1] == 0)
    def _():
        all_ref[:, :half] = own_ref[...]
        all_ref[:, half:] = far_ref[...]

    @pl.when(place[1] != 0)
    def _():
        all_ref[:, :half] = far_ref[...]
        all_ref[:, half:] = own_ref[...]

    pieces = (own, below, w_low, w_high, above)
    for o in range(X):
        at = slice(W * o, W * o + W)
        for k in range(D // W):
            d_second = all_ref[:, W * k : W * k + W]
            more = dot(d_second, rows_of(pieces, D + W * k, W)[o], ((1,), (1,)))
            back_ref[...] = more if k == 0 else back_ref[...] + more
        tanh = tanh_ref[:, at]
        d1_ref[:, at] = (back_ref[...] * (1.0 - tanh * tanh)).astype(BF)
    put_sums((low, high), 2, in_ref, tanh_ref, all_ref, d1_ref, wt_ref, inc_ref)


def small_kernel(place, error, coef, factor, inc_ref, out):
    scale = 1.0 / math.sqrt(inc_ref.shape[0] * Y * Z)
    err = error[...]
    adjoint = 2.0 * scale * err * coef[...]
    rows = inc_ref.shape[0] // 2
    for i in range(2):
        more = lax.dot_general(
            jnp.broadcast_to(adjoint[i : i + 1, :], (8, rows)),
            inc_ref[rows * i : rows * (i + 1), :],
            (((1,), (0,)), ((), ())),
            precision=lax.Precision.HIGHEST,
            preferred_element_type=F32,
        )
        grad_z = more if i == 0 else grad_z + more
    loss = scale * jnp.sum(err * err)
    grad_y = jnp.sum(adjoint * factor[...])
    row = lax.broadcasted_iota(jnp.int32, (8, W), 0)
    lane = lax.broadcasted_iota(jnp.int32, (8, W), 1)
    scalars = jnp.where(lane == 0, loss, jnp.where(lane == 1, grad_y, 0.0))
    out[...] = jnp.where(row == 0, grad_z, jnp.where(row == 1, scalars, 0.0))


def own_kernel(place, in_ref, tanh_ref, all_ref, d1_ref, wt_ref, inc_ref, out, token):
    token[...] = jnp.zeros_like(token)
    put_sums((out,), 0, in_ref, tanh_ref, all_ref, d1_ref, wt_ref, inc_ref)


def near_kernel(
    place, in_ref, tanh_ref, all_ref, d1_ref, wt_ref, inc_ref, from_low, from_high, token, small, up, down
):
    rest = (in_ref, tanh_ref, all_ref, d1_ref, wt_ref, inc_ref)
    put_sums((up,), 3, *rest, (from_low, range(Z // 2)))
    put_sums((down,), 1, *rest, (from_high, range(Z // 2, Z)))


def sum_x_kernel(place, own, from_below, from_above, small_ref, *outs):
    rows = own.shape[1]
    small = two_words(small_ref[...])
    for r, out in enumerate(outs):
        k = lax.rem(place[3] + r, Z)
        out[:rows, :] = (
            own[k].astype(F32) + from_below[k].astype(F32) + from_above[k].astype(F32)
        ).astype(BF)
        out[rows:, :] = small


def sum_z_kernel(place, *refs):
    p, out, far = refs[:Z], refs[Z], refs[Z + 1]

    def total(row, rows):
        v = [ref[row : row + rows, :].astype(F32) for ref in p]
        return ((v[0] + v[4]) + (v[2] + v[6])) + ((v[1] + v[5]) + (v[3] + v[7]))

    for row in range(0, 320, 64):
        out[row : row + 64, :] = total(row, 64).astype(BF)
    far[...] = total(320, 64).astype(BF)
    words = total(384, 16)
    out[320:, :] = two_words(words[:8] + words[8:])


def pieces_kernel(place, main, far, out):
    out[:256, :] = main[:256, :]
    c = place[1]
    out[pl.ds(pl.multiple_of(256 + 64 * c, 64), 64), :] = main[256:320, :]
    out[pl.ds(pl.multiple_of(256 + 64 * (1 - c), 64), 64), :] = far[...]
    out[384:, :] = main[320:, :]


def out_kernel(place, own, below, above, low, high, first, second, third, loss, grad_y, grad_z):
    y = place[2]
    parts = [(own, 0, k, k) for k in range(Z)]
    parts += [(below, Y - 1, k, k) for k in range(Z)] + [(above, 1, k, k) for k in range(Z)]
    parts += [(low, 2, k, k) for k in range(Z // 2)]
    parts += [(high, 2, k, k + Z // 2) for k in range(Z // 2)]
    for ref, off, i, k in parts:
        at = lax.rem(y + off, Y)
        first[at, k] = ref[i, :128, :]
        second[at, :, W * k : W * k + W] = ref[i, 128:256, :]
        third[at, 0, k] = ref[i, 256:320, :]
        third[at, 1, k] = ref[i, 320:384, :]

    def words(ref):
        both = ref[0, 384:, :].astype(F32)
        return both[:8] + both[8:]

    small = (words(own) + words(low)) + (words(below) + words(above))
    grad_z[...] = small[0:1, :]
    loss[...] = small[1:2, 0:1]
    grad_y[...] = small[1:2, 1:2]


def factors_of(default_step, steps):
    counter = jnp.arange(steps, dtype=F32)
    factors = (
        1.0
        + DISCOUNT / steps
        - DEFAULT_LOSS * (counter[:, None] == default_step[None, :]).astype(F32)
    )
    coefs = [jnp.ones(default_step.shape, F32)]
    for n in range(steps - 1, 0, -1):
        coefs.append(coefs[-1] * factors[n])
    return factors, jnp.stack(coefs[::-1])


def local(
    x_start, y_start, z_start, increments, default_step, term_weight, w_first, w_second, w_third
):
    steps, paths, width = increments.shape
    tstep = 1.0 / steps
    scale = 1.0 / math.sqrt(paths * Y * Z)
    x, c, y, z = (lax.axis_index(name) for name in ("x", "core", "y", "z"))
    place = jnp.stack([x, c, y, z]).astype(jnp.int32)
    half = D // CORES
    flat = (2, paths // 2)

    third = w_third.reshape(X, CORES, half, width)
    far_third = core_swap(lax.dynamic_slice(third, (y, 1 - c, 0, 0), (1, 1, half, width))[0, 0])
    hbm, vmem = (pl.BlockSpec(memory_space=space) for space in (pltpu.HBM, pltpu.VMEM))
    packed = pl.pallas_call(
        pack_kernel,
        out_shape=jax.ShapeDtypeStruct((3 * D, width), BF),
        in_specs=[pl.BlockSpec(memory_space=pltpu.SMEM), hbm, hbm, hbm, vmem],
        out_specs=vmem,
        scratch_shapes=[pltpu.SemaphoreType.DMA((2 + D // W,))],
        name="pack_kernel",
    )(place, w_first, w_second, third, far_third)
    increments, packed = lax.optimization_barrier((increments, packed))

    states = x_start[None, :] * (1.0 + DRIFT_RATE * tstep + VOLATILITY * increments[0])
    sends = []
    for n in range(1, steps):
        sends.append(jnp.stack([states.astype(BF), increments[n].astype(BF)]))
        states = states * (1.0 + DRIFT_RATE * tstep + VOLATILITY * increments[n])
    sends = jnp.stack(sends)
    rows = [pick(sends, y)] + [y_plus(pick(sends, (y + r) % Y), r) for r in range(1, Y)]
    step_here = default_step.astype(F32)
    factors_here, coefs_here = factors_of(step_here, steps)
    target_part = jnp.sum(states * term_weight[None, :], axis=1) / math.sqrt(D)
    first_part = jnp.sum(increments[0] * z_start[None, :], axis=1)
    there = jnp.concatenate(
        [(coefs_here[0] * first_part - target_part).reshape(flat), step_here.reshape(flat)]
    )
    rows, there = lax.optimization_barrier((rows, there))
    rows = jnp.stack(rows)
    near = [pick(rows, (y - x + X) % X)]
    near += [x_plus(pick(rows, (y - x - q + 2 * X) % X), q) for q in range(1, X)]
    below, above = x_plus(packed, 1), x_plus(packed, 3)
    mid = 3 * D // 2
    low = x_plus(below[:mid], 1)
    high = x_plus(above[mid:], 3)
    weights = (packed, below, low, high, above)
    near = jnp.stack(near)
    far = core_swap(near)
    there = turned(there)

    inputs, incs = vmem_call(
        arrange_kernel, place, (near, far), (((paths, D), BF), ((paths, D), BF))
    )
    tanh_first, mine, other = vmem_call(
        forward_kernel,
        place,
        (inputs, *weights),
        [((paths, half), F32)] * 3,
        [pltpu.VMEM((paths, D), F32)],
    )
    there, _ = lax.optimization_barrier((there, mine))
    part_sum = there[:2]
    factors, coefs = factors_of(there[2:].reshape(paths), steps)
    other = core_swap(other)
    (back,) = vmem_call(back_kernel, place, (incs, *weights), [((paths, half), F32)])
    tanh_second = jnp.tanh(mine + other)
    dots = jnp.sum(tanh_second * back, axis=1)
    coef = pick(coefs, y + 1)
    total = part_sum + (coef * dots).reshape(flat)
    total = total + core_swap(total)
    others = [y_plus(total, r) for r in range(1, Y)]
    total = (total + others[1]) + (others[0] + others[2])
    total = total + (factors[0] * coefs[0] * y_start).reshape(flat)
    adjoint = 2.0 * scale * total.reshape(paths)

    weight = (adjoint * coef)[:, None]
    weighted = (weight * tanh_second).astype(BF)
    d_second = (weight * back * (1.0 - tanh_second * tanh_second)).astype(BF)
    d_far = core_swap(d_second)
    low, high, d_all, d_first, sent = vmem_call(
        far_kernel,
        place,
        (inputs, tanh_first, d_second, d_far, *weights, weighted, incs, total),
        (
            ((Z // 2, 384, width), BF),
            ((Z // 2, 384, width), BF),
            ((paths, D), BF),
            ((paths, half), BF),
            (flat, F32),
        ),
        [pltpu.VMEM((paths, width), F32)],
    )
    (small,) = vmem_call(
        small_kernel,
        place,
        (turned(sent), coefs_here[0].reshape(flat), factors_here[0].reshape(flat), increments[0]),
        (((8, width), F32),),
    )
    low, high = x_plus(low, 1), x_plus(high, 3)
    shared = (inputs, tanh_first, d_all, d_first, weighted, incs)
    piece = ((Z, 384, width), BF)
    own, token = vmem_call(own_kernel, place, shared, (piece, ((8, width), F32)))
    up, down = vmem_call(
        near_kernel, place, (*shared, low, high, token, small), (piece, piece)
    )
    up, down = x_plus(up, 1), x_plus(down, 3)
    parts = vmem_call(
        sum_x_kernel, place, (own, up, down, small), [((400, width), BF)] * Z
    )
    arrived = {r: z_plus(parts[r], r) for r in (3, 5, 4, 2, 6, 1, 7)}
    parts = [parts[0]] + [arrived[r] for r in range(1, Z)]
    main, far = vmem_call(
        sum_z_kernel, place, parts, (((336, width), BF), ((64, width), BF))
    )
    (pieces,) = vmem_call(pieces_kernel, place, (main, core_swap(far)), (((400, width), BF),))
    own = lax.all_gather(pieces, "z")
    below, above = y_plus(own, 1), y_plus(own, 3)
    low, high = y_plus(below[: Z // 2], 1), y_plus(above[Z // 2 :], 3)
    first, second, third, loss, grad_y, grad_z = vmem_call(
        out_kernel,
        place,
        (own, below, above, low, high),
        (
            ((X, Z, 128, width), BF),
            ((X, 128, D), BF),
            ((X, CORES, Z, 64, width), BF),
            ((1, 1), F32),
            ((1, 1), F32),
            ((1, width), F32),
        ),
    )
    return (
        loss[0, 0],
        grad_y[0, 0],
        grad_z[0],
        first.reshape(X, D, width),
        second,
        third.reshape(X, D, width),
    )


def solution(mesh):
    axes = Mesh(mesh.devices.reshape(Z, Y, X, CORES), ("z", "y", "x", "core"))
    batch, dim = ("z", "y"), ("x", "core")
    placed = (
        P(dim),
        P(),
        P(dim),
        P(None, batch, dim),
        P(batch),
        P(dim),
        P(None, None, dim),
        P(None, dim, None),
        P(None, None, dim),
    )

    return jax.shard_map(
        local,
        mesh=axes,
        in_specs=placed,
        out_specs=(
            P(),
            P(),
            P(dim),
            P(None, None, dim),
            P(None, dim, None),
            P(None, None, dim),
        ),
        check_vma=False,
    )
```

```python
import math

import jax
import jax.numpy as jnp
from jax import lax
from jax.experimental import pallas as pl
from jax.experimental.pallas import tpu as pltpu
from jax.sharding import Mesh
from jax.sharding import PartitionSpec as P


D = 1024

DRIFT_RATE = 0.06
VOLATILITY = 0.2
DISCOUNT = 0.02
DEFAULT_LOSS = 1.0 / 3.0

X, CORES, Y, Z = 4, 2, 4, 8
STEPS = 5
W = D // (X * CORES)
ROOM = 20 << 20
BF = jnp.bfloat16
F32 = jnp.float32


def shifted(value, axis, n, o):
    return lax.ppermute(value, axis, [(i, (i + o) % n) for i in range(n)])


def flipped(value, axis, n, bit):
    return lax.ppermute(value, axis, [(i, i ^ bit) for i in range(n)])


def x_plus(value, o):
    return shifted(value, "x", X, o)


def y_plus(value, o):
    return shifted(value, "y", Y, o)


def z_plus(value, o):
    return shifted(value, "z", Z, o)


def turned(value):
    pairs = [(X * y + x, X * x + y) for y in range(Y) for x in range(X)]
    return lax.ppermute(value, ("y", "x"), pairs)


def core_swap(value):
    return flipped(value, "core", CORES, 1)


def pick(array, index):
    return lax.dynamic_index_in_dim(array, index, 0, keepdims=False)


def dot(a, b, contract):
    return lax.dot_general(a, b, (contract, ((), ())), preferred_element_type=F32)


def vmem_call(kernel, place, args, outs, scratch=()):
    vmem = pl.BlockSpec(memory_space=pltpu.VMEM)
    return pl.pallas_call(
        kernel,
        out_shape=[jax.ShapeDtypeStruct(shape, dtype) for shape, dtype in outs],
        in_specs=[pl.BlockSpec(memory_space=pltpu.SMEM)] + [vmem] * len(args),
        out_specs=[vmem] * len(outs),
        scratch_shapes=list(scratch),
        compiler_params=pltpu.CompilerParams(vmem_limit_bytes=ROOM),
    )(place, *args)


def two_words(value):
    high = value.astype(BF).astype(F32)
    return jnp.concatenate([high, value - high], axis=0).astype(BF)


def arrange_kernel(place, near, far, inputs, incs):
    x, c = place[0], place[1]
    for i in range(X):
        r = lax.rem(x + (X - i), X)
        inputs[:, pl.ds(pl.multiple_of(2 * W * i + W * c, W), W)] = near[r, 0]
        inputs[:, pl.ds(pl.multiple_of(2 * W * i + W * (1 - c), W), W)] = far[r, 0]
        incs[:, 2 * W * i : 2 * W * i + W] = near[i, 1]
        incs[:, 2 * W * i + W : 2 * W * i + 2 * W] = far[i, 1]


def pack_kernel(place, first, second, third, far, out, sems):
    c, y = place[1], place[2]
    half = far.shape[0]
    copies = [
        (first.at[y], out.at[:D, :]),
        (third.at[y, c], out.at[2 * D : 2 * D + half, :]),
    ]
    for k in range(D // W):
        copies.append((second.at[y, :, pl.ds(W * k, W)], out.at[D + W * k : D + W * k + W, :]))
    copies = [pltpu.make_async_copy(a, b, sems.at[i]) for i, (a, b) in enumerate(copies)]
    for copy in copies:
        copy.start()
    out[2 * D + half :, :] = far[...]
    for copy in copies:
        copy.wait()


def rows_of(pieces, row, rows):
    own, below, low, high, above = pieces
    mid = low.shape[0]
    apart = low[row : row + rows, :] if row < mid else high[row - mid : row - mid + rows, :]
    return [own[row : row + rows, :], below[row : row + rows, :], apart, above[row : row + rows, :]]


def forward_kernel(place, in_ref, own, below, low, high, above, tanh_ref, mine, other, part):
    pieces = (own, below, low, high, above)
    for o, first in enumerate(rows_of(pieces, 0, D)):
        tanh_ref[:, W * o : W * o + W] = jnp.tanh(dot(in_ref[...], first, ((1,), (0,))))
    for o in range(X):
        hidden = tanh_ref[:, W * o : W * o + W].astype(BF)
        for k in range(D // W):
            at = slice(W * k, W * k + W)
            more = dot(hidden, rows_of(pieces, D + W * k, W)[o], ((1,), (0,)))
            part[:, at] = more if o == 0 else part[:, at] + more
    half = mine.shape[1]

    @pl.when(place[1] == 0)
    def _():
        mine[...] = part[:, :half]
        other[...] = part[:, half:]

    @pl.when(place[1] != 0)
    def _():
        mine[...] = part[:, half:]
        other[...] = part[:, :half]


def back_kernel(place, inc_ref, own, below, low, high, above, out):
    half = out.shape[1]
    pieces = (own, below, low, high, above)
    for i in range(CORES):
        for o, piece in enumerate(rows_of(pieces, 2 * D + half * i, half)):
            at = W * (CORES * o + i)
            more = dot(inc_ref[:, at : at + W], piece, ((1,), (1,)))
            out[...] = more if i + o == 0 else out[...] + more


def loss_kernel(place, mine, other, back, there, tanh_ref, total, coef_ref):
    tanh = jnp.tanh(mine[...] + other[...])
    tanh_ref[...] = tanh
    sums = lax.dot_general(
        jnp.ones((8, tanh.shape[1]), F32),
        tanh * back[...],
        (((1,), (1,)), ((), ())),
        precision=lax.Precision.HIGHEST,
        preferred_element_type=F32,
    )
    row = lax.broadcasted_iota(jnp.int32, (2, W), 0)
    dots = jnp.where(row == 0, sums[:2, :W], sums[:2, W:])
    step = there[2:4, :]
    coef = jnp.ones((2, W), F32)
    for n in range(STEPS - 1, 1, -1):
        factor = 1.0 + DISCOUNT / STEPS - DEFAULT_LOSS * jnp.where(step == float(n), 1.0, 0.0)
        coef = jnp.where(place[2] + 1 < n, coef * factor, coef)
    coef_ref[...] = coef
    total[...] = there[:2, :] + coef * dots


def add_kernel(place, a, b, out):
    out[...] = a[...] + b[...]


def weigh_kernel(place, own, p1, p2, p3, coef, tanh_ref, back, weighted, d_second, error):
    scale = 1.0 / math.sqrt(tanh_ref.shape[0] * Y * Z)
    err = (own[...] + p2[...]) + (p1[...] + p3[...])
    error[...] = err
    adjoint = 2.0 * scale * err * coef[...]
    for i in range(2):
        at = slice(W * i, W * i + W)
        column = jnp.transpose(jnp.broadcast_to(adjoint[i : i + 1, :], (W, W)))
        for q in range(0, tanh_ref.shape[1], W):
            tanh = tanh_ref[at, q : q + W]
            weighted[at, q : q + W] = (column * tanh).astype(BF)
            more = column * back[at, q : q + W] * (1.0 - tanh * tanh)
            d_second[at, q : q + W] = more.astype(BF)


def put_sums(outs, o, in_ref, tanh_ref, all_ref, d1_ref, wt_ref, inc_ref, added=None):
    at = slice(W * o, W * o + W)
    g1 = dot(in_ref[...], d1_ref[:, at], ((0,), (0,)))
    g2 = dot(tanh_ref[:, at].astype(BF), all_ref[...], ((0,), (0,)))
    g3 = dot(wt_ref[...], inc_ref[:, 2 * W * o : 2 * W * o + 2 * W], ((0,), (0,)))
    share = Z // len(outs)

    def put(k, row, value):
        rows = value.shape[0]
        if added is not None and k in added[1]:
            value = value + added[0][k - added[1][0], row : row + rows, :].astype(F32)
        outs[k // share][k % share, row : row + rows, :] = value.astype(BF)

    for k in range(Z):
        put(k, 0, g1[W * k : W * k + W])
        put(k, 128, g2[:, W * k : W * k + W])
        put(k, 256, g3[64 * k : 64 * k + 64, :W])
        put(k, 320, g3[64 * k : 64 * k + 64, W:])


def far_kernel(
    place, in_ref, tanh_ref, own_ref, far_ref, own, below, w_low, w_high, above, wt_ref, inc_ref,
    error, low, high, all_ref, d1_ref, sent, back_ref
):
    sent[...] = error[...]
    half = own_ref.shape[1]

    @pl.when(place[1] == 0)
    def _():
        all_ref[:, :half] = own_ref[...]
        all_ref[:, half:] = far_ref[...]

    @pl.when(place[1] != 0)
    def _():
        all_ref[:, :half] = far_ref[...]
        all_ref[:, half:] = own_ref[...]

    pieces = (own, below, w_low, w_high, above)
    for o in range(X):
        at = slice(W * o, W * o + W)
        for k in range(D // W):
            d_second = all_ref[:, W * k : W * k + W]
            more = dot(d_second, rows_of(pieces, D + W * k, W)[o], ((1,), (1,)))
            back_ref[...] = more if k == 0 else back_ref[...] + more
        tanh = tanh_ref[:, at]
        d1_ref[:, at] = (back_ref[...] * (1.0 - tanh * tanh)).astype(BF)
    put_sums((low, high), 2, in_ref, tanh_ref, all_ref, d1_ref, wt_ref, inc_ref)


def small_kernel(place, error, coef, factor, inc_ref, out):
    scale = 1.0 / math.sqrt(inc_ref.shape[0] * Y * Z)
    err = error[...]
    adjoint = 2.0 * scale * err * coef[...]
    rows = inc_ref.shape[0] // 2
    for i in range(2):
        more = lax.dot_general(
            jnp.broadcast_to(adjoint[i : i + 1, :], (8, rows)),
            inc_ref[rows * i : rows * (i + 1), :],
            (((1,), (0,)), ((), ())),
            precision=lax.Precision.HIGHEST,
            preferred_element_type=F32,
        )
        grad_z = more if i == 0 else grad_z + more
    loss = scale * jnp.sum(err * err)
    grad_y = jnp.sum(adjoint * factor[...])
    row = lax.broadcasted_iota(jnp.int32, (8, W), 0)
    lane = lax.broadcasted_iota(jnp.int32, (8, W), 1)
    scalars = jnp.where(lane == 0, loss, jnp.where(lane == 1, grad_y, 0.0))
    out[...] = jnp.where(row == 0, grad_z, jnp.where(row == 1, scalars, 0.0))


def own_kernel(place, in_ref, tanh_ref, all_ref, d1_ref, wt_ref, inc_ref, out, token):
    token[...] = jnp.zeros_like(token)
    put_sums((out,), 0, in_ref, tanh_ref, all_ref, d1_ref, wt_ref, inc_ref)


def near_kernel(
    place, in_ref, tanh_ref, all_ref, d1_ref, wt_ref, inc_ref, from_low, from_high, token, small, up, down
):
    rest = (in_ref, tanh_ref, all_ref, d1_ref, wt_ref, inc_ref)
    put_sums((up,), 3, *rest, (from_low, range(Z // 2)))
    put_sums((down,), 1, *rest, (from_high, range(Z // 2, Z)))


def sum_x_kernel(place, own, from_below, from_above, small_ref, *outs):
    rows = own.shape[1]
    small = two_words(small_ref[...])
    for r, out in enumerate(outs):
        k = lax.rem(place[3] + r, Z)
        out[:rows, :] = (
            own[k].astype(F32) + from_below[k].astype(F32) + from_above[k].astype(F32)
        ).astype(BF)
        out[rows:, :] = small


def sum_z_kernel(place, *refs):
    p, out, far = refs[:Z], refs[Z], refs[Z + 1]

    def total(row, rows):
        v = [ref[row : row + rows, :].astype(F32) for ref in p]
        return ((v[0] + v[4]) + (v[2] + v[6])) + ((v[1] + v[5]) + (v[3] + v[7]))

    for row in range(0, 320, 64):
        out[row : row + 64, :] = total(row, 64).astype(BF)
    far[...] = total(320, 64).astype(BF)
    words = total(384, 16)
    out[320:, :] = two_words(words[:8] + words[8:])


def pieces_kernel(place, main, far, out):
    out[:256, :] = main[:256, :]
    c = place[1]
    out[pl.ds(pl.multiple_of(256 + 64 * c, 64), 64), :] = main[256:320, :]
    out[pl.ds(pl.multiple_of(256 + 64 * (1 - c), 64), 64), :] = far[...]
    out[384:, :] = main[320:, :]


def out_kernel(place, own, below, above, low, high, first, second, third, loss, grad_y, grad_z):
    y = place[2]
    parts = [(own, 0, k, k) for k in range(Z)]
    parts += [(below, Y - 1, k, k) for k in range(Z)] + [(above, 1, k, k) for k in range(Z)]
    parts += [(low, 2, k, k) for k in range(Z // 2)]
    parts += [(high, 2, k, k + Z // 2) for k in range(Z // 2)]
    for ref, off, i, k in parts:
        at = lax.rem(y + off, Y)
        first[at, k] = ref[i, :128, :]
        second[at, :, W * k : W * k + W] = ref[i, 128:256, :]
        third[at, 0, k] = ref[i, 256:320, :]
        third[at, 1, k] = ref[i, 320:384, :]

    def words(ref):
        both = ref[0, 384:, :].astype(F32)
        return both[:8] + both[8:]

    small = (words(own) + words(low)) + (words(below) + words(above))
    grad_z[...] = small[0:1, :]
    loss[...] = small[1:2, 0:1]
    grad_y[...] = small[1:2, 1:2]


def factors_of(default_step, steps):
    counter = jnp.arange(steps, dtype=F32)
    factors = (
        1.0
        + DISCOUNT / steps
        - DEFAULT_LOSS * (counter[:, None] == default_step[None, :]).astype(F32)
    )
    coefs = [jnp.ones(default_step.shape, F32)]
    for n in range(steps - 1, 0, -1):
        coefs.append(coefs[-1] * factors[n])
    return factors, jnp.stack(coefs[::-1])


def local(
    x_start, y_start, z_start, increments, default_step, term_weight, w_first, w_second, w_third
):
    steps, paths, width = increments.shape
    tstep = 1.0 / steps
    x, c, y, z = (lax.axis_index(name) for name in ("x", "core", "y", "z"))
    place = jnp.stack([x, c, y, z]).astype(jnp.int32)
    half = D // CORES
    flat = (2, paths // 2)

    third = w_third.reshape(X, CORES, half, width)
    far_third = core_swap(lax.dynamic_slice(third, (y, 1 - c, 0, 0), (1, 1, half, width))[0, 0])
    hbm, vmem = (pl.BlockSpec(memory_space=space) for space in (pltpu.HBM, pltpu.VMEM))
    packed = pl.pallas_call(
        pack_kernel,
        out_shape=jax.ShapeDtypeStruct((3 * D, width), BF),
        in_specs=[pl.BlockSpec(memory_space=pltpu.SMEM), hbm, hbm, hbm, vmem],
        out_specs=vmem,
        scratch_shapes=[pltpu.SemaphoreType.DMA((2 + D // W,))],
        name="pack_kernel",
    )(place, w_first, w_second, third, far_third)
    increments, packed = lax.optimization_barrier((increments, packed))

    states = x_start[None, :] * (1.0 + DRIFT_RATE * tstep + VOLATILITY * increments[0])
    sends = []
    for n in range(1, steps):
        sends.append(jnp.stack([states.astype(BF), increments[n].astype(BF)]))
        states = states * (1.0 + DRIFT_RATE * tstep + VOLATILITY * increments[n])
    sends = jnp.stack(sends)
    rows = [pick(sends, y)] + [y_plus(pick(sends, (y + r) % Y), r) for r in range(1, Y)]
    step_here = default_step.astype(F32)
    factors_here, coefs_here = factors_of(step_here, steps)
    target_part = jnp.sum(states * term_weight[None, :], axis=1) / math.sqrt(D)
    first_part = jnp.sum(increments[0] * z_start[None, :], axis=1)
    start = factors_here[0] * coefs_here[0] * y_start / (X * CORES)
    there = jnp.concatenate(
        [(coefs_here[0] * first_part - target_part + start).reshape(flat), step_here.reshape(flat)]
    )
    rows, there = lax.optimization_barrier((rows, there))
    rows = jnp.stack(rows)
    near = [pick(rows, (y - x + X) % X)]
    near += [x_plus(pick(rows, (y - x - q + 2 * X) % X), q) for q in range(1, X)]
    below, above = x_plus(packed, 1), x_plus(packed, 3)
    mid = 3 * D // 2
    low = x_plus(below[:mid], 1)
    high = x_plus(above[mid:], 3)
    weights = (packed, below, low, high, above)
    near = jnp.stack(near)
    far = core_swap(near)
    there = turned(there)

    inputs, incs = vmem_call(
        arrange_kernel, place, (near, far), (((paths, D), BF), ((paths, D), BF))
    )
    tanh_first, mine, other = vmem_call(
        forward_kernel,
        place,
        (inputs, *weights),
        [((paths, half), F32)] * 3,
        [pltpu.VMEM((paths, D), F32)],
    )
    other = core_swap(other)
    (back,) = vmem_call(back_kernel, place, (incs, *weights), [((paths, half), F32)])
    tanh_second, total, coef = vmem_call(
        loss_kernel,
        place,
        (mine, other, back, there),
        (((paths, half), F32), (flat, F32), (flat, F32)),
    )
    (total,) = vmem_call(add_kernel, place, (total, core_swap(total)), ((flat, F32),))
    others = [y_plus(total, r) for r in range(1, Y)]

    weighted, d_second, error = vmem_call(
        weigh_kernel,
        place,
        (total, *others, coef, tanh_second, back),
        (((paths, half), BF), ((paths, half), BF), (flat, F32)),
    )
    d_far = core_swap(d_second)
    low, high, d_all, d_first, sent = vmem_call(
        far_kernel,
        place,
        (inputs, tanh_first, d_second, d_far, *weights, weighted, incs, error),
        (
            ((Z // 2, 384, width), BF),
            ((Z // 2, 384, width), BF),
            ((paths, D), BF),
            ((paths, half), BF),
            (flat, F32),
        ),
        [pltpu.VMEM((paths, width), F32)],
    )
    (small,) = vmem_call(
        small_kernel,
        place,
        (turned(sent), coefs_here[0].reshape(flat), factors_here[0].reshape(flat), increments[0]),
        (((8, width), F32),),
    )
    low, high = x_plus(low, 1), x_plus(high, 3)
    shared = (inputs, tanh_first, d_all, d_first, weighted, incs)
    piece = ((Z, 384, width), BF)
    own, token = vmem_call(own_kernel, place, shared, (piece, ((8, width), F32)))
    up, down = vmem_call(
        near_kernel, place, (*shared, low, high, token, small), (piece, piece)
    )
    up, down = x_plus(up, 1), x_plus(down, 3)
    parts = vmem_call(
        sum_x_kernel, place, (own, up, down, small), [((400, width), BF)] * Z
    )
    arrived = {}
    for r in range(1, Z):
        arrived[r] = z_plus(parts[r], r)
    parts = [parts[0]] + [arrived[r] for r in range(1, Z)]
    main, far = vmem_call(
        sum_z_kernel, place, parts, (((336, width), BF), ((64, width), BF))
    )
    (pieces,) = vmem_call(pieces_kernel, place, (main, core_swap(far)), (((400, width), BF),))
    own = lax.all_gather(pieces, "z")
    below, above = y_plus(own, 1), y_plus(own, 3)
    low, high = y_plus(below[: Z // 2], 1), y_plus(above[Z // 2 :], 3)
    first, second, third, loss, grad_y, grad_z = vmem_call(
        out_kernel,
        place,
        (own, below, above, low, high),
        (
            ((X, Z, 128, width), BF),
            ((X, 128, D), BF),
            ((X, CORES, Z, 64, width), BF),
            ((1, 1), F32),
            ((1, 1), F32),
            ((1, width), F32),
        ),
    )
    return (
        loss[0, 0],
        grad_y[0, 0],
        grad_z[0],
        first.reshape(X, D, width),
        second,
        third.reshape(X, D, width),
    )


def solution(mesh):
    axes = Mesh(mesh.devices.reshape(Z, Y, X, CORES), ("z", "y", "x", "core"))
    batch, dim = ("z", "y"), ("x", "core")
    placed = (
        P(dim),
        P(),
        P(dim),
        P(None, batch, dim),
        P(batch),
        P(dim),
        P(None, None, dim),
        P(None, dim, None),
        P(None, None, dim),
    )

    return jax.shard_map(
        local,
        mesh=axes,
        in_specs=placed,
        out_specs=(
            P(),
            P(),
            P(dim),
            P(None, None, dim),
            P(None, dim, None),
            P(None, None, dim),
        ),
        check_vma=False,
    )
```

```python
import math

import jax
import jax.numpy as jnp
from jax import lax
from jax.experimental import pallas as pl
from jax.experimental.pallas import tpu as pltpu
from jax.sharding import Mesh
from jax.sharding import PartitionSpec as P


D = 1024

DRIFT_RATE = 0.06
VOLATILITY = 0.2
DISCOUNT = 0.02
DEFAULT_LOSS = 1.0 / 3.0

X, CORES, Y, Z = 4, 2, 4, 8
STEPS = 5
W = D // (X * CORES)
ROOM = 20 << 20
BF = jnp.bfloat16
F32 = jnp.float32


def shifted(value, axis, n, o):
    return lax.ppermute(value, axis, [(i, (i + o) % n) for i in range(n)])


def flipped(value, axis, n, bit):
    return lax.ppermute(value, axis, [(i, i ^ bit) for i in range(n)])


def x_plus(value, o):
    return shifted(value, "x", X, o)


def y_plus(value, o):
    return shifted(value, "y", Y, o)


def z_plus(value, o):
    return shifted(value, "z", Z, o)


def turned(value):
    pairs = [(X * y + x, X * x + y) for y in range(Y) for x in range(X)]
    return lax.ppermute(value, ("y", "x"), pairs)


def core_swap(value):
    return flipped(value, "core", CORES, 1)


def pick(array, index):
    return lax.dynamic_index_in_dim(array, index, 0, keepdims=False)


def dot(a, b, contract):
    return lax.dot_general(a, b, (contract, ((), ())), preferred_element_type=F32)


def vmem_call(kernel, place, args, outs, scratch=()):
    vmem = pl.BlockSpec(memory_space=pltpu.VMEM)
    return pl.pallas_call(
        kernel,
        out_shape=[jax.ShapeDtypeStruct(shape, dtype) for shape, dtype in outs],
        in_specs=[pl.BlockSpec(memory_space=pltpu.SMEM)] + [vmem] * len(args),
        out_specs=[vmem] * len(outs),
        scratch_shapes=list(scratch),
        compiler_params=pltpu.CompilerParams(vmem_limit_bytes=ROOM),
    )(place, *args)


def two_words(value):
    high = value.astype(BF).astype(F32)
    return jnp.concatenate([high, value - high], axis=0).astype(BF)


def arrange_kernel(place, near, far, inputs, incs):
    x, c = place[0], place[1]
    for i in range(X):
        r = lax.rem(x + (X - i), X)
        inputs[:, pl.ds(pl.multiple_of(2 * W * i + W * c, W), W)] = near[r, 0]
        inputs[:, pl.ds(pl.multiple_of(2 * W * i + W * (1 - c), W), W)] = far[r, 0]
        incs[:, 2 * W * i : 2 * W * i + W] = near[i, 1]
        incs[:, 2 * W * i + W : 2 * W * i + 2 * W] = far[i, 1]


def pack_kernel(place, first, second, third, far, out, sems):
    c, y = place[1], place[2]
    half = far.shape[0]
    copies = [
        (first.at[y], out.at[:D, :]),
        (third.at[y, c], out.at[2 * D : 2 * D + half, :]),
    ]
    for k in range(D // W):
        copies.append((second.at[y, :, pl.ds(W * k, W)], out.at[D + W * k : D + W * k + W, :]))
    copies = [pltpu.make_async_copy(a, b, sems.at[i]) for i, (a, b) in enumerate(copies)]
    for copy in copies:
        copy.start()
    out[2 * D + half :, :] = far[...]
    for copy in copies:
        copy.wait()


def rows_of(pieces, row, rows):
    own, below, low, high, above = pieces
    mid = low.shape[0]
    apart = low[row : row + rows, :] if row < mid else high[row - mid : row - mid + rows, :]
    return [own[row : row + rows, :], below[row : row + rows, :], apart, above[row : row + rows, :]]


def forward_kernel(place, in_ref, own, below, low, high, above, tanh_ref, mine, other, part):
    pieces = (own, below, low, high, above)
    for o, first in enumerate(rows_of(pieces, 0, D)):
        tanh_ref[:, W * o : W * o + W] = jnp.tanh(dot(in_ref[...], first, ((1,), (0,))))
    for o in range(X):
        hidden = tanh_ref[:, W * o : W * o + W].astype(BF)
        for k in range(D // W):
            at = slice(W * k, W * k + W)
            more = dot(hidden, rows_of(pieces, D + W * k, W)[o], ((1,), (0,)))
            part[:, at] = more if o == 0 else part[:, at] + more
    half = mine.shape[1]

    @pl.when(place[1] == 0)
    def _():
        mine[...] = part[:, :half]
        other[...] = part[:, half:]

    @pl.when(place[1] != 0)
    def _():
        mine[...] = part[:, half:]
        other[...] = part[:, :half]


def back_kernel(place, inc_ref, own, below, low, high, above, out):
    half = out.shape[1]
    pieces = (own, below, low, high, above)
    for i in range(CORES):
        for o, piece in enumerate(rows_of(pieces, 2 * D + half * i, half)):
            at = W * (CORES * o + i)
            more = dot(inc_ref[:, at : at + W], piece, ((1,), (1,)))
            out[...] = more if i + o == 0 else out[...] + more


def loss_kernel(place, mine, other, back, there, tanh_ref, total, coef_ref):
    tanh = jnp.tanh(mine[...] + other[...])
    tanh_ref[...] = tanh
    sums = lax.dot_general(
        jnp.ones((8, tanh.shape[1]), F32),
        tanh * back[...],
        (((1,), (1,)), ((), ())),
        precision=lax.Precision.HIGHEST,
        preferred_element_type=F32,
    )
    row = lax.broadcasted_iota(jnp.int32, (2, W), 0)
    dots = jnp.where(row == 0, sums[:2, :W], sums[:2, W:])
    step = there[2:4, :]
    coef = jnp.ones((2, W), F32)
    for n in range(STEPS - 1, 1, -1):
        factor = 1.0 + DISCOUNT / STEPS - DEFAULT_LOSS * jnp.where(step == float(n), 1.0, 0.0)
        coef = jnp.where(place[2] + 1 < n, coef * factor, coef)
    coef_ref[...] = coef
    total[...] = there[:2, :] + coef * dots


def add_kernel(place, a, b, out):
    out[...] = a[...] + b[...]


def weigh_kernel(place, own, p1, p2, p3, coef, tanh_ref, back, weighted, d_second, error):
    scale = 1.0 / math.sqrt(tanh_ref.shape[0] * Y * Z)
    err = (own[...] + p2[...]) + (p1[...] + p3[...])
    error[...] = err
    adjoint = 2.0 * scale * err * coef[...]
    for i in range(2):
        at = slice(W * i, W * i + W)
        column = jnp.transpose(jnp.broadcast_to(adjoint[i : i + 1, :], (W, W)))
        for q in range(0, tanh_ref.shape[1], W):
            tanh = tanh_ref[at, q : q + W]
            weighted[at, q : q + W] = (column * tanh).astype(BF)
            more = column * back[at, q : q + W] * (1.0 - tanh * tanh)
            d_second[at, q : q + W] = more.astype(BF)


def put_sums(outs, o, in_ref, tanh_ref, all_ref, d1_ref, wt_ref, inc_ref, added=None):
    at = slice(W * o, W * o + W)
    g1 = dot(in_ref[...], d1_ref[:, at], ((0,), (0,)))
    g2 = dot(tanh_ref[:, at].astype(BF), all_ref[...], ((0,), (0,)))
    g3 = dot(wt_ref[...], inc_ref[:, 2 * W * o : 2 * W * o + 2 * W], ((0,), (0,)))
    share = Z // len(outs)

    def put(k, row, value):
        rows = value.shape[0]
        if added is not None and k in added[1]:
            value = value + added[0][k - added[1][0], row : row + rows, :].astype(F32)
        outs[k // share][k % share, row : row + rows, :] = value.astype(BF)

    for k in range(Z):
        put(k, 0, g1[W * k : W * k + W])
        put(k, 128, g2[:, W * k : W * k + W])
        put(k, 256, g3[64 * k : 64 * k + 64, :W])
        put(k, 320, g3[64 * k : 64 * k + 64, W:])


def far_kernel(
    place, in_ref, tanh_ref, own_ref, far_ref, own, below, w_low, w_high, above, wt_ref, inc_ref,
    error, low, high, all_ref, d1_ref, sent, back_ref
):
    sent[...] = error[...]
    half = own_ref.shape[1]

    @pl.when(place[1] == 0)
    def _():
        all_ref[:, :half] = own_ref[...]
        all_ref[:, half:] = far_ref[...]

    @pl.when(place[1] != 0)
    def _():
        all_ref[:, :half] = far_ref[...]
        all_ref[:, half:] = own_ref[...]

    pieces = (own, below, w_low, w_high, above)
    for o in range(X):
        at = slice(W * o, W * o + W)
        for k in range(D // W):
            d_second = all_ref[:, W * k : W * k + W]
            more = dot(d_second, rows_of(pieces, D + W * k, W)[o], ((1,), (1,)))
            back_ref[...] = more if k == 0 else back_ref[...] + more
        tanh = tanh_ref[:, at]
        d1_ref[:, at] = (back_ref[...] * (1.0 - tanh * tanh)).astype(BF)
    put_sums((low, high), 2, in_ref, tanh_ref, all_ref, d1_ref, wt_ref, inc_ref)


def small_kernel(place, error, coef, factor, inc_ref, out):
    scale = 1.0 / math.sqrt(inc_ref.shape[0] * Y * Z)
    err = error[...]
    adjoint = 2.0 * scale * err * coef[...]
    rows = inc_ref.shape[0] // 2
    for i in range(2):
        more = lax.dot_general(
            jnp.broadcast_to(adjoint[i : i + 1, :], (8, rows)),
            inc_ref[rows * i : rows * (i + 1), :],
            (((1,), (0,)), ((), ())),
            precision=lax.Precision.HIGHEST,
            preferred_element_type=F32,
        )
        grad_z = more if i == 0 else grad_z + more
    loss = scale * jnp.sum(err * err)
    grad_y = jnp.sum(adjoint * factor[...])
    row = lax.broadcasted_iota(jnp.int32, (8, W), 0)
    lane = lax.broadcasted_iota(jnp.int32, (8, W), 1)
    scalars = jnp.where(lane == 0, loss, jnp.where(lane == 1, grad_y, 0.0))
    out[...] = jnp.where(row == 0, grad_z, jnp.where(row == 1, scalars, 0.0))


def own_kernel(place, in_ref, tanh_ref, all_ref, d1_ref, wt_ref, inc_ref, out, token):
    token[...] = jnp.zeros_like(token)
    put_sums((out,), 0, in_ref, tanh_ref, all_ref, d1_ref, wt_ref, inc_ref)


def near_kernel(
    place, in_ref, tanh_ref, all_ref, d1_ref, wt_ref, inc_ref, from_low, from_high, token, small, up, down
):
    rest = (in_ref, tanh_ref, all_ref, d1_ref, wt_ref, inc_ref)
    put_sums((up,), 3, *rest, (from_low, range(Z // 2)))
    put_sums((down,), 1, *rest, (from_high, range(Z // 2, Z)))


def sum_x_kernel(place, own, from_below, from_above, small_ref, *outs):
    rows = own.shape[1]
    small = two_words(small_ref[...])
    for r, out in enumerate(outs):
        k = lax.rem(place[3] + r, Z)
        out[:rows, :] = (
            own[k].astype(F32) + from_below[k].astype(F32) + from_above[k].astype(F32)
        ).astype(BF)
        out[rows:, :] = small


def sum_z_kernel(place, *refs):
    p, out, far = refs[:Z], refs[Z], refs[Z + 1]

    def total(row, rows):
        v = [ref[row : row + rows, :].astype(F32) for ref in p]
        return ((v[0] + v[4]) + (v[2] + v[6])) + ((v[1] + v[5]) + (v[3] + v[7]))

    for row in range(0, 320, 64):
        out[row : row + 64, :] = total(row, 64).astype(BF)
    far[...] = total(320, 64).astype(BF)
    words = total(384, 16)
    out[320:, :] = two_words(words[:8] + words[8:])


def pieces_kernel(place, main, far, out):
    out[:256, :] = main[:256, :]
    c = place[1]
    out[pl.ds(pl.multiple_of(256 + 64 * c, 64), 64), :] = main[256:320, :]
    out[pl.ds(pl.multiple_of(256 + 64 * (1 - c), 64), 64), :] = far[...]
    out[384:, :] = main[320:, :]


NEAR, FAR, CUT = (6, 7, 0, 1, 2), (3, 4, 5), 208


def stack_kernel(place, *refs):
    for i, ref in enumerate(refs[:-1]):
        refs[-1][i] = ref[...]


def stack_far_kernel(place, a3, a5, low, high, out):
    out[0] = a3[...]
    out[1, :CUT, :] = low[...]
    out[1, CUT:, :] = high[...]
    out[2] = a5[...]


def out_kernel(
    place, own, own_far, below, below_far, above, above_far, apart, apart_far,
    first, second, third, loss, grad_y, grad_z
):
    y, z = place[2], place[3]
    parts = ((own, own_far, 0), (below, below_far, Y - 1), (above, above_far, 1), (apart, apart_far, 2))
    for near, far, off in parts:
        at = lax.rem(y + off, Y)
        for ref, shifts in ((near, NEAR), (far, FAR)):

            def place_one(i, carry, ref=ref, shift=shifts[0], at=at):
                k = lax.rem(z + (2 * Z - shift) - i, Z)
                first[at, k] = ref[i, :128, :]
                second[at, :, pl.ds(pl.multiple_of(W * k, W), W)] = ref[i, 128:256, :]
                third[at, 0, k] = ref[i, 256:320, :]
                third[at, 1, k] = ref[i, 320:384, :]
                return carry

            lax.fori_loop(0, len(shifts), place_one, 0)

    def words(ref):
        both = ref[0, 384:, :].astype(F32)
        return both[:8] + both[8:]

    small = (words(own) + words(apart)) + (words(below) + words(above))
    grad_z[...] = small[0:1, :]
    loss[...] = small[1:2, 0:1]
    grad_y[...] = small[1:2, 1:2]


def factors_of(default_step, steps):
    counter = jnp.arange(steps, dtype=F32)
    factors = (
        1.0
        + DISCOUNT / steps
        - DEFAULT_LOSS * (counter[:, None] == default_step[None, :]).astype(F32)
    )
    coefs = [jnp.ones(default_step.shape, F32)]
    for n in range(steps - 1, 0, -1):
        coefs.append(coefs[-1] * factors[n])
    return factors, jnp.stack(coefs[::-1])


def local(
    x_start, y_start, z_start, increments, default_step, term_weight, w_first, w_second, w_third
):
    steps, paths, width = increments.shape
    tstep = 1.0 / steps
    x, c, y, z = (lax.axis_index(name) for name in ("x", "core", "y", "z"))
    place = jnp.stack([x, c, y, z]).astype(jnp.int32)
    half = D // CORES
    flat = (2, paths // 2)

    third = w_third.reshape(X, CORES, half, width)
    far_third = core_swap(lax.dynamic_slice(third, (y, 1 - c, 0, 0), (1, 1, half, width))[0, 0])
    hbm, vmem = (pl.BlockSpec(memory_space=space) for space in (pltpu.HBM, pltpu.VMEM))
    packed = pl.pallas_call(
        pack_kernel,
        out_shape=jax.ShapeDtypeStruct((3 * D, width), BF),
        in_specs=[pl.BlockSpec(memory_space=pltpu.SMEM), hbm, hbm, hbm, vmem],
        out_specs=vmem,
        scratch_shapes=[pltpu.SemaphoreType.DMA((2 + D // W,))],
        name="pack_kernel",
    )(place, w_first, w_second, third, far_third)
    increments, packed = lax.optimization_barrier((increments, packed))

    states = x_start[None, :] * (1.0 + DRIFT_RATE * tstep + VOLATILITY * increments[0])
    sends = []
    for n in range(1, steps):
        sends.append(jnp.stack([states.astype(BF), increments[n].astype(BF)]))
        states = states * (1.0 + DRIFT_RATE * tstep + VOLATILITY * increments[n])
    sends = jnp.stack(sends)
    rows = [pick(sends, y)] + [y_plus(pick(sends, (y + r) % Y), r) for r in range(1, Y)]
    step_here = default_step.astype(F32)
    factors_here, coefs_here = factors_of(step_here, steps)
    target_part = jnp.sum(states * term_weight[None, :], axis=1) / math.sqrt(D)
    first_part = jnp.sum(increments[0] * z_start[None, :], axis=1)
    start = factors_here[0] * coefs_here[0] * y_start / (X * CORES)
    there = jnp.concatenate(
        [(coefs_here[0] * first_part - target_part + start).reshape(flat), step_here.reshape(flat)]
    )
    rows, there = lax.optimization_barrier((rows, there))
    rows = jnp.stack(rows)
    near = [pick(rows, (y - x + X) % X)]
    near += [x_plus(pick(rows, (y - x - q + 2 * X) % X), q) for q in range(1, X)]
    below, above = x_plus(packed, 1), x_plus(packed, 3)
    mid = 3 * D // 2
    low = x_plus(below[:mid], 1)
    high = x_plus(above[mid:], 3)
    weights = (packed, below, low, high, above)
    near = jnp.stack(near)
    far = core_swap(near)
    there = turned(there)

    inputs, incs = vmem_call(
        arrange_kernel, place, (near, far), (((paths, D), BF), ((paths, D), BF))
    )
    tanh_first, mine, other = vmem_call(
        forward_kernel,
        place,
        (inputs, *weights),
        [((paths, half), F32)] * 3,
        [pltpu.VMEM((paths, D), F32)],
    )
    other = core_swap(other)
    (back,) = vmem_call(back_kernel, place, (incs, *weights), [((paths, half), F32)])
    tanh_second, total, coef = vmem_call(
        loss_kernel,
        place,
        (mine, other, back, there),
        (((paths, half), F32), (flat, F32), (flat, F32)),
    )
    (total,) = vmem_call(add_kernel, place, (total, core_swap(total)), ((flat, F32),))
    others = [y_plus(total, r) for r in range(1, Y)]

    weighted, d_second, error = vmem_call(
        weigh_kernel,
        place,
        (total, *others, coef, tanh_second, back),
        (((paths, half), BF), ((paths, half), BF), (flat, F32)),
    )
    d_far = core_swap(d_second)
    low, high, d_all, d_first, sent = vmem_call(
        far_kernel,
        place,
        (inputs, tanh_first, d_second, d_far, *weights, weighted, incs, error),
        (
            ((Z // 2, 384, width), BF),
            ((Z // 2, 384, width), BF),
            ((paths, D), BF),
            ((paths, half), BF),
            (flat, F32),
        ),
        [pltpu.VMEM((paths, width), F32)],
    )
    (small,) = vmem_call(
        small_kernel,
        place,
        (turned(sent), coefs_here[0].reshape(flat), factors_here[0].reshape(flat), increments[0]),
        (((8, width), F32),),
    )
    low, high = x_plus(low, 1), x_plus(high, 3)
    shared = (inputs, tanh_first, d_all, d_first, weighted, incs)
    piece = ((Z, 384, width), BF)
    own, token = vmem_call(own_kernel, place, shared, (piece, ((8, width), F32)))
    up, down = vmem_call(
        near_kernel, place, (*shared, low, high, token, small), (piece, piece)
    )
    up, down = x_plus(up, 1), x_plus(down, 3)
    parts = vmem_call(
        sum_x_kernel, place, (own, up, down, small), [((400, width), BF)] * Z
    )
    arrived = {}
    for r in range(1, Z):
        arrived[r] = z_plus(parts[r], r)
    parts = [parts[0]] + [arrived[r] for r in range(1, Z)]
    main, far = vmem_call(
        sum_z_kernel, place, parts, (((336, width), BF), ((64, width), BF))
    )
    (pieces,) = vmem_call(pieces_kernel, place, (main, core_swap(far)), (((400, width), BF),))
    gathered = {0: pieces}
    for r in (2, 6, 1, 7):
        gathered[r] = z_plus(pieces, r)
    (own,) = vmem_call(
        stack_kernel,
        place,
        [gathered[r] for r in NEAR],
        (((len(NEAR), 400, width), BF),),
    )
    below = y_plus(own, 1)
    above = y_plus(own, 3)
    low = z_plus(gathered[2][:CUT], 2)
    high = z_plus(gathered[6][CUT:], 6)
    gathered[3] = z_plus(gathered[2], 1)
    gathered[5] = z_plus(gathered[6], 7)
    (own_far,) = vmem_call(
        stack_far_kernel,
        place,
        (gathered[3], gathered[5], low, high),
        (((len(FAR), 400, width), BF),),
    )
    below_far, above_far = y_plus(own_far, 1), y_plus(own_far, 3)
    apart, apart_far = y_plus(below, 1), y_plus(above_far, 3)
    first, second, third, loss, grad_y, grad_z = vmem_call(
        out_kernel,
        place,
        (own, own_far, below, below_far, above, above_far, apart, apart_far),
        (
            ((X, Z, 128, width), BF),
            ((X, 128, D), BF),
            ((X, CORES, Z, 64, width), BF),
            ((1, 1), F32),
            ((1, 1), F32),
            ((1, width), F32),
        ),
    )
    return (
        loss[0, 0],
        grad_y[0, 0],
        grad_z[0],
        first.reshape(X, D, width),
        second,
        third.reshape(X, D, width),
    )


def solution(mesh):
    axes = Mesh(mesh.devices.reshape(Z, Y, X, CORES), ("z", "y", "x", "core"))
    batch, dim = ("z", "y"), ("x", "core")
    placed = (
        P(dim),
        P(),
        P(dim),
        P(None, batch, dim),
        P(batch),
        P(dim),
        P(None, None, dim),
        P(None, dim, None),
        P(None, None, dim),
    )

    return jax.shard_map(
        local,
        mesh=axes,
        in_specs=placed,
        out_specs=(
            P(),
            P(),
            P(dim),
            P(None, None, dim),
            P(None, dim, None),
            P(None, None, dim),
        ),
        check_vma=False,
    )
```

```python
import math

import jax
import jax.numpy as jnp
from jax import lax
from jax.experimental import pallas as pl
from jax.experimental.pallas import tpu as pltpu
from jax.sharding import Mesh
from jax.sharding import PartitionSpec as P


D = 1024

DRIFT_RATE = 0.06
VOLATILITY = 0.2
DISCOUNT = 0.02
DEFAULT_LOSS = 1.0 / 3.0

X, CORES, Y, Z = 4, 2, 4, 8
STEPS = 5
W = D // (X * CORES)
ROOM = 20 << 20
BF = jnp.bfloat16
F32 = jnp.float32


def shifted(value, axis, n, o):
    return lax.ppermute(value, axis, [(i, (i + o) % n) for i in range(n)])


def flipped(value, axis, n, bit):
    return lax.ppermute(value, axis, [(i, i ^ bit) for i in range(n)])


def x_plus(value, o):
    return shifted(value, "x", X, o)


def y_plus(value, o):
    return shifted(value, "y", Y, o)


def z_plus(value, o):
    return shifted(value, "z", Z, o)


def turned(value):
    pairs = [(X * y + x, X * x + y) for y in range(Y) for x in range(X)]
    return lax.ppermute(value, ("y", "x"), pairs)


def core_swap(value):
    return flipped(value, "core", CORES, 1)


def pick(array, index):
    return lax.dynamic_index_in_dim(array, index, 0, keepdims=False)


def dot(a, b, contract):
    return lax.dot_general(a, b, (contract, ((), ())), preferred_element_type=F32)


def vmem_call(kernel, place, args, outs, scratch=()):
    vmem = pl.BlockSpec(memory_space=pltpu.VMEM)
    return pl.pallas_call(
        kernel,
        out_shape=[jax.ShapeDtypeStruct(shape, dtype) for shape, dtype in outs],
        in_specs=[pl.BlockSpec(memory_space=pltpu.SMEM)] + [vmem] * len(args),
        out_specs=[vmem] * len(outs),
        scratch_shapes=list(scratch),
        compiler_params=pltpu.CompilerParams(vmem_limit_bytes=ROOM),
    )(place, *args)


def two_words(value):
    high = value.astype(BF).astype(F32)
    return jnp.concatenate([high, value - high], axis=0).astype(BF)


def arrange_kernel(place, near, far, inputs, incs):
    x, c = place[0], place[1]
    for i in range(X):
        r = lax.rem(x + (X - i), X)
        inputs[:, pl.ds(pl.multiple_of(2 * W * i + W * c, W), W)] = near[r, 0]
        inputs[:, pl.ds(pl.multiple_of(2 * W * i + W * (1 - c), W), W)] = far[r, 0]
        incs[:, 2 * W * i : 2 * W * i + W] = near[i, 1]
        incs[:, 2 * W * i + W : 2 * W * i + 2 * W] = far[i, 1]


def pack_kernel(place, first, second, third, far, out, sems):
    c, y = place[1], place[2]
    half = far.shape[0]
    copies = [
        (first.at[y], out.at[:D, :]),
        (third.at[y, c], out.at[2 * D : 2 * D + half, :]),
    ]
    for k in range(D // W):
        copies.append((second.at[y, :, pl.ds(W * k, W)], out.at[D + W * k : D + W * k + W, :]))
    copies = [pltpu.make_async_copy(a, b, sems.at[i]) for i, (a, b) in enumerate(copies)]
    for copy in copies:
        copy.start()
    out[2 * D + half :, :] = far[...]
    for copy in copies:
        copy.wait()


def rows_of(pieces, row, rows):
    own, below, low, high, above = pieces
    mid = low.shape[0]
    apart = low[row : row + rows, :] if row < mid else high[row - mid : row - mid + rows, :]
    return [own[row : row + rows, :], below[row : row + rows, :], apart, above[row : row + rows, :]]


def forward_kernel(place, in_ref, own, below, low, high, above, tanh_ref, mine, other, part):
    pieces = (own, below, low, high, above)
    for o, first in enumerate(rows_of(pieces, 0, D)):
        tanh_ref[:, W * o : W * o + W] = jnp.tanh(dot(in_ref[...], first, ((1,), (0,))))
    for o in range(X):
        hidden = tanh_ref[:, W * o : W * o + W].astype(BF)
        for k in range(D // W):
            at = slice(W * k, W * k + W)
            more = dot(hidden, rows_of(pieces, D + W * k, W)[o], ((1,), (0,)))
            part[:, at] = more if o == 0 else part[:, at] + more
    half = mine.shape[1]

    @pl.when(place[1] == 0)
    def _():
        mine[...] = part[:, :half]
        other[...] = part[:, half:]

    @pl.when(place[1] != 0)
    def _():
        mine[...] = part[:, half:]
        other[...] = part[:, :half]


def back_kernel(place, inc_ref, own, below, low, high, above, out):
    half = out.shape[1]
    pieces = (own, below, low, high, above)
    for i in range(CORES):
        for o, piece in enumerate(rows_of(pieces, 2 * D + half * i, half)):
            at = W * (CORES * o + i)
            more = dot(inc_ref[:, at : at + W], piece, ((1,), (1,)))
            out[...] = more if i + o == 0 else out[...] + more


def loss_kernel(place, mine, other, back, there, tanh_ref, total, coef_ref):
    tanh = jnp.tanh(mine[...] + other[...])
    tanh_ref[...] = tanh
    sums = lax.dot_general(
        jnp.ones((8, tanh.shape[1]), F32),
        tanh * back[...],
        (((1,), (1,)), ((), ())),
        precision=lax.Precision.HIGHEST,
        preferred_element_type=F32,
    )
    row = lax.broadcasted_iota(jnp.int32, (2, W), 0)
    dots = jnp.where(row == 0, sums[:2, :W], sums[:2, W:])
    step = there[2:4, :]
    coef = jnp.ones((2, W), F32)
    for n in range(STEPS - 1, 1, -1):
        factor = 1.0 + DISCOUNT / STEPS - DEFAULT_LOSS * jnp.where(step == float(n), 1.0, 0.0)
        coef = jnp.where(place[2] + 1 < n, coef * factor, coef)
    coef_ref[...] = coef
    total[...] = there[:2, :] + coef * dots


def add_kernel(place, a, b, out):
    out[...] = a[...] + b[...]


def weigh_kernel(place, own, p1, p2, p3, coef, tanh_ref, back, weighted, d_second, error):
    scale = 1.0 / math.sqrt(tanh_ref.shape[0] * Y * Z)
    err = (own[...] + p2[...]) + (p1[...] + p3[...])
    error[...] = err
    adjoint = 2.0 * scale * err * coef[...]
    for i in range(2):
        at = slice(W * i, W * i + W)
        column = jnp.transpose(jnp.broadcast_to(adjoint[i : i + 1, :], (W, W)))
        for q in range(0, tanh_ref.shape[1], W):
            tanh = tanh_ref[at, q : q + W]
            weighted[at, q : q + W] = (column * tanh).astype(BF)
            more = column * back[at, q : q + W] * (1.0 - tanh * tanh)
            d_second[at, q : q + W] = more.astype(BF)


def put_sums(outs, o, in_ref, tanh_ref, all_ref, d1_ref, wt_ref, inc_ref, added=None):
    at = slice(W * o, W * o + W)
    g1 = dot(in_ref[...], d1_ref[:, at], ((0,), (0,)))
    g2 = dot(tanh_ref[:, at].astype(BF), all_ref[...], ((0,), (0,)))
    g3 = dot(wt_ref[...], inc_ref[:, 2 * W * o : 2 * W * o + 2 * W], ((0,), (0,)))
    share = Z // len(outs)

    def put(k, row, value):
        rows = value.shape[0]
        if added is not None and k in added[1]:
            value = value + added[0][k - added[1][0], row : row + rows, :].astype(F32)
        outs[k // share][k % share, row : row + rows, :] = value.astype(BF)

    for k in range(Z):
        put(k, 0, g1[W * k : W * k + W])
        put(k, 128, g2[:, W * k : W * k + W])
        put(k, 256, g3[64 * k : 64 * k + 64, :W])
        put(k, 320, g3[64 * k : 64 * k + 64, W:])


def far_kernel(
    place, in_ref, tanh_ref, own_ref, far_ref, own, below, w_low, w_high, above, wt_ref, inc_ref,
    error, low, high, all_ref, d1_ref, sent, back_ref
):
    sent[...] = error[...]
    half = own_ref.shape[1]

    @pl.when(place[1] == 0)
    def _():
        all_ref[:, :half] = own_ref[...]
        all_ref[:, half:] = far_ref[...]

    @pl.when(place[1] != 0)
    def _():
        all_ref[:, :half] = far_ref[...]
        all_ref[:, half:] = own_ref[...]

    pieces = (own, below, w_low, w_high, above)
    for o in range(X):
        at = slice(W * o, W * o + W)
        for k in range(D // W):
            d_second = all_ref[:, W * k : W * k + W]
            more = dot(d_second, rows_of(pieces, D + W * k, W)[o], ((1,), (1,)))
            back_ref[...] = more if k == 0 else back_ref[...] + more
        tanh = tanh_ref[:, at]
        d1_ref[:, at] = (back_ref[...] * (1.0 - tanh * tanh)).astype(BF)
    put_sums((low, high), 2, in_ref, tanh_ref, all_ref, d1_ref, wt_ref, inc_ref)


def small_kernel(place, error, coef, factor, inc_ref, out):
    scale = 1.0 / math.sqrt(inc_ref.shape[0] * Y * Z)
    err = error[...]
    adjoint = 2.0 * scale * err * coef[...]
    rows = inc_ref.shape[0] // 2
    for i in range(2):
        more = lax.dot_general(
            jnp.broadcast_to(adjoint[i : i + 1, :], (8, rows)),
            inc_ref[rows * i : rows * (i + 1), :],
            (((1,), (0,)), ((), ())),
            precision=lax.Precision.HIGHEST,
            preferred_element_type=F32,
        )
        grad_z = more if i == 0 else grad_z + more
    loss = scale * jnp.sum(err * err)
    grad_y = jnp.sum(adjoint * factor[...])
    row = lax.broadcasted_iota(jnp.int32, (8, W), 0)
    lane = lax.broadcasted_iota(jnp.int32, (8, W), 1)
    scalars = jnp.where(lane == 0, loss, jnp.where(lane == 1, grad_y, 0.0))
    out[...] = jnp.where(row == 0, grad_z, jnp.where(row == 1, scalars, 0.0))


def own_kernel(place, in_ref, tanh_ref, all_ref, d1_ref, wt_ref, inc_ref, out, token):
    token[...] = jnp.zeros_like(token)
    put_sums((out,), 0, in_ref, tanh_ref, all_ref, d1_ref, wt_ref, inc_ref)


def near_kernel(
    place, in_ref, tanh_ref, all_ref, d1_ref, wt_ref, inc_ref, from_low, from_high, token, small, up, down
):
    rest = (in_ref, tanh_ref, all_ref, d1_ref, wt_ref, inc_ref)
    put_sums((up,), 3, *rest, (from_low, range(Z // 2)))
    put_sums((down,), 1, *rest, (from_high, range(Z // 2, Z)))


def sum_x_kernel(place, own, from_below, from_above, small_ref, out):
    rows = own.shape[1]
    small = two_words(small_ref[...])

    def add(i, carry):
        at = pl.ds(pl.multiple_of(64 * i, 64), 64)
        for k in range(Z):
            out[k, at, :] = (
                own[k, at, :].astype(F32)
                + from_below[k, at, :].astype(F32)
                + from_above[k, at, :].astype(F32)
            ).astype(BF)
        return carry

    lax.fori_loop(0, rows // 64, add, 0)
    for k in range(Z):
        out[k, rows:, :] = small


def sum_z_kernel(place, got, out, far):

    def total(row, rows):
        v = [got[k, pl.ds(row, rows), :].astype(F32) for k in range(Z)]
        return ((v[0] + v[4]) + (v[2] + v[6])) + ((v[1] + v[5]) + (v[3] + v[7]))

    def add(i, carry):
        row = pl.multiple_of(64 * i, 64)
        out[pl.ds(row, 64), :] = total(row, 64).astype(BF)
        return carry

    lax.fori_loop(0, 5, add, 0)
    far[...] = total(320, 64).astype(BF)
    words = total(384, 16)
    out[320:, :] = two_words(words[:8] + words[8:])


def pieces_kernel(place, main, far, out):
    out[:256, :] = main[:256, :]
    c = place[1]
    out[pl.ds(pl.multiple_of(256 + 64 * c, 64), 64), :] = main[256:320, :]
    out[pl.ds(pl.multiple_of(256 + 64 * (1 - c), 64), 64), :] = far[...]
    out[384:, :] = main[320:, :]


NEAR, FAR, CUT = (6, 7, 0, 1, 2), (3, 4, 5), 208


def stack_kernel(place, *refs):
    for i, ref in enumerate(refs[:-1]):
        refs[-1][i] = ref[...]


def stack_far_kernel(place, a3, a5, low, high, out):
    out[0] = a3[...]
    out[1, :CUT, :] = low[...]
    out[1, CUT:, :] = high[...]
    out[2] = a5[...]


def out_kernel(
    place, own, own_far, below, below_far, above, above_far, apart, apart_far,
    first, second, third, loss, grad_y, grad_z
):
    y, z = place[2], place[3]
    parts = ((own, own_far, 0), (below, below_far, Y - 1), (above, above_far, 1), (apart, apart_far, 2))
    for near, far, off in parts:
        at = lax.rem(y + off, Y)
        for ref, shifts in ((near, NEAR), (far, FAR)):

            def place_one(i, carry, ref=ref, shift=shifts[0], at=at):
                k = lax.rem(z + (2 * Z - shift) - i, Z)
                first[at, k] = ref[i, :128, :]
                second[at, :, pl.ds(pl.multiple_of(W * k, W), W)] = ref[i, 128:256, :]
                third[at, 0, k] = ref[i, 256:320, :]
                third[at, 1, k] = ref[i, 320:384, :]
                return carry

            lax.fori_loop(0, len(shifts), place_one, 0)

    def words(ref):
        both = ref[0, 384:, :].astype(F32)
        return both[:8] + both[8:]

    small = (words(own) + words(apart)) + (words(below) + words(above))
    grad_z[...] = small[0:1, :]
    loss[...] = small[1:2, 0:1]
    grad_y[...] = small[1:2, 1:2]


def factors_of(default_step, steps):
    counter = jnp.arange(steps, dtype=F32)
    factors = (
        1.0
        + DISCOUNT / steps
        - DEFAULT_LOSS * (counter[:, None] == default_step[None, :]).astype(F32)
    )
    coefs = [jnp.ones(default_step.shape, F32)]
    for n in range(steps - 1, 0, -1):
        coefs.append(coefs[-1] * factors[n])
    return factors, jnp.stack(coefs[::-1])


def local(
    x_start, y_start, z_start, increments, default_step, term_weight, w_first, w_second, w_third
):
    steps, paths, width = increments.shape
    tstep = 1.0 / steps
    x, c, y, z = (lax.axis_index(name) for name in ("x", "core", "y", "z"))
    place = jnp.stack([x, c, y, z]).astype(jnp.int32)
    half = D // CORES
    flat = (2, paths // 2)

    third = w_third.reshape(X, CORES, half, width)
    far_third = core_swap(lax.dynamic_slice(third, (y, 1 - c, 0, 0), (1, 1, half, width))[0, 0])
    hbm, vmem = (pl.BlockSpec(memory_space=space) for space in (pltpu.HBM, pltpu.VMEM))
    packed = pl.pallas_call(
        pack_kernel,
        out_shape=jax.ShapeDtypeStruct((3 * D, width), BF),
        in_specs=[pl.BlockSpec(memory_space=pltpu.SMEM), hbm, hbm, hbm, vmem],
        out_specs=vmem,
        scratch_shapes=[pltpu.SemaphoreType.DMA((2 + D // W,))],
        name="pack_kernel",
    )(place, w_first, w_second, third, far_third)
    increments, packed = lax.optimization_barrier((increments, packed))

    states = x_start[None, :] * (1.0 + DRIFT_RATE * tstep + VOLATILITY * increments[0])
    sends = []
    for n in range(1, steps):
        sends.append(jnp.stack([states.astype(BF), increments[n].astype(BF)]))
        states = states * (1.0 + DRIFT_RATE * tstep + VOLATILITY * increments[n])
    sends = jnp.stack(sends)
    rows = [pick(sends, y)] + [y_plus(pick(sends, (y + r) % Y), r) for r in range(1, Y)]
    step_here = default_step.astype(F32)
    factors_here, coefs_here = factors_of(step_here, steps)
    target_part = jnp.sum(states * term_weight[None, :], axis=1) / math.sqrt(D)
    first_part = jnp.sum(increments[0] * z_start[None, :], axis=1)
    start = factors_here[0] * coefs_here[0] * y_start / (X * CORES)
    there = jnp.concatenate(
        [(coefs_here[0] * first_part - target_part + start).reshape(flat), step_here.reshape(flat)]
    )
    rows, there = lax.optimization_barrier((rows, there))
    rows = jnp.stack(rows)
    near = [pick(rows, (y - x + X) % X)]
    near += [x_plus(pick(rows, (y - x - q + 2 * X) % X), q) for q in range(1, X)]
    below, above = x_plus(packed, 1), x_plus(packed, 3)
    mid = 3 * D // 2
    low = x_plus(below[:mid], 1)
    high = x_plus(above[mid:], 3)
    weights = (packed, below, low, high, above)
    near = jnp.stack(near)
    far = core_swap(near)
    there = turned(there)

    inputs, incs = vmem_call(
        arrange_kernel, place, (near, far), (((paths, D), BF), ((paths, D), BF))
    )
    tanh_first, mine, other = vmem_call(
        forward_kernel,
        place,
        (inputs, *weights),
        [((paths, half), F32)] * 3,
        [pltpu.VMEM((paths, D), F32)],
    )
    other = core_swap(other)
    (back,) = vmem_call(back_kernel, place, (incs, *weights), [((paths, half), F32)])
    tanh_second, total, coef = vmem_call(
        loss_kernel,
        place,
        (mine, other, back, there),
        (((paths, half), F32), (flat, F32), (flat, F32)),
    )
    (total,) = vmem_call(add_kernel, place, (total, core_swap(total)), ((flat, F32),))
    others = [y_plus(total, r) for r in range(1, Y)]

    weighted, d_second, error = vmem_call(
        weigh_kernel,
        place,
        (total, *others, coef, tanh_second, back),
        (((paths, half), BF), ((paths, half), BF), (flat, F32)),
    )
    d_far = core_swap(d_second)
    low, high, d_all, d_first, sent = vmem_call(
        far_kernel,
        place,
        (inputs, tanh_first, d_second, d_far, *weights, weighted, incs, error),
        (
            ((Z // 2, 384, width), BF),
            ((Z // 2, 384, width), BF),
            ((paths, D), BF),
            ((paths, half), BF),
            (flat, F32),
        ),
        [pltpu.VMEM((paths, width), F32)],
    )
    (small,) = vmem_call(
        small_kernel,
        place,
        (turned(sent), coefs_here[0].reshape(flat), factors_here[0].reshape(flat), increments[0]),
        (((8, width), F32),),
    )
    low, high = x_plus(low, 1), x_plus(high, 3)
    shared = (inputs, tanh_first, d_all, d_first, weighted, incs)
    piece = ((Z, 384, width), BF)
    own, token = vmem_call(own_kernel, place, shared, (piece, ((8, width), F32)))
    up, down = vmem_call(
        near_kernel, place, (*shared, low, high, token, small), (piece, piece)
    )
    up, down = x_plus(up, 1), x_plus(down, 3)
    (parts,) = vmem_call(
        sum_x_kernel, place, (own, up, down, small), (((Z, 400, width), BF),)
    )
    parts = lax.all_to_all(parts, "z", split_axis=0, concat_axis=0, tiled=True)
    main, far = vmem_call(
        sum_z_kernel, place, (parts,), (((336, width), BF), ((64, width), BF))
    )
    (pieces,) = vmem_call(pieces_kernel, place, (main, core_swap(far)), (((400, width), BF),))
    gathered = {0: pieces}
    for r in (2, 6, 1, 7):
        gathered[r] = z_plus(pieces, r)
    (own,) = vmem_call(
        stack_kernel,
        place,
        [gathered[r] for r in NEAR],
        (((len(NEAR), 400, width), BF),),
    )
    below = y_plus(own, 1)
    above = y_plus(own, 3)
    low = z_plus(gathered[2][:CUT], 2)
    high = z_plus(gathered[6][CUT:], 6)
    gathered[3] = z_plus(gathered[2], 1)
    gathered[5] = z_plus(gathered[6], 7)
    (own_far,) = vmem_call(
        stack_far_kernel,
        place,
        (gathered[3], gathered[5], low, high),
        (((len(FAR), 400, width), BF),),
    )
    below_far, above_far = y_plus(own_far, 1), y_plus(own_far, 3)
    apart, apart_far = y_plus(below, 1), y_plus(above_far, 3)
    first, second, third, loss, grad_y, grad_z = vmem_call(
        out_kernel,
        place,
        (own, own_far, below, below_far, above, above_far, apart, apart_far),
        (
            ((X, Z, 128, width), BF),
            ((X, 128, D), BF),
            ((X, CORES, Z, 64, width), BF),
            ((1, 1), F32),
            ((1, 1), F32),
            ((1, width), F32),
        ),
    )
    return (
        loss[0, 0],
        grad_y[0, 0],
        grad_z[0],
        first.reshape(X, D, width),
        second,
        third.reshape(X, D, width),
    )


def solution(mesh):
    axes = Mesh(mesh.devices.reshape(Z, Y, X, CORES), ("z", "y", "x", "core"))
    batch, dim = ("z", "y"), ("x", "core")
    placed = (
        P(dim),
        P(),
        P(dim),
        P(None, batch, dim),
        P(batch),
        P(dim),
        P(None, None, dim),
        P(None, dim, None),
        P(None, None, dim),
    )

    return jax.shard_map(
        local,
        mesh=axes,
        in_specs=placed,
        out_specs=(
            P(),
            P(),
            P(dim),
            P(None, None, dim),
            P(None, dim, None),
            P(None, None, dim),
        ),
        check_vma=False,
    )
```
